128 devices in a mesh: grp: 2 (over z_hi), dev: 64 (over x, z_lo, y, core).
Axes of the slice: x: 4, y: 4, z: 4 (z_hi: 2, z_lo: 2; z = z_hi * 2 + z_lo), core: 2. Of those that a mesh axis runs over, the one named last changes fastest.
Arguments:
- inputs: bfloat16 [256, 196, 1024], P(('grp', 'dev')), may hold values from -6 to 6
- cotangent: bfloat16 [256, 196, 1024], P(('grp', 'dev')), may hold values from -24 to 24
- first_gain: float32 [1024], replicated, may hold values from 0.5 to 1.5
- first_shift: float32 [1024], replicated, may hold values from -3 to 3
- token_in: bfloat16 [512, 196], replicated, may hold values from -0.4375 to 0.4375
- token_in_bias: float32 [512], replicated, may hold values from -3 to 3
- token_out: bfloat16 [512, 196], replicated, may hold values from -0.25 to 0.25
- second_gain: float32 [1024], replicated, may hold values from 0.5 to 1.5
- second_shift: float32 [1024], replicated, may hold values from -3 to 3
- channel_in: bfloat16 [1024, 4096], replicated, may hold values from -0.1875 to 0.1875
- channel_in_bias: float32 [4096], replicated, may hold values from -3 to 3
- channel_out: bfloat16 [1024, 4096], replicated, may hold values from -0.09375 to 0.09375
Outputs:
- grad_inputs: bfloat16 [256, 196, 1024], P(('grp', 'dev'))
- grad_token_in: float32 [512, 196], P('dev')
- grad_token_out: float32 [512, 196], P('dev')
- grad_channel_in: float32 [1024, 4096], P('dev')
- grad_channel_out: float32 [1024, 4096], P('dev')
- grad_norms: float32 [5, 1024], replicated
- grad_token_in_bias: float32 [512], replicated
- grad_token_out_bias: float32 [196], replicated
- grad_channel_in_bias: float32 [4096], replicated
The draws below stay inside these ranges and needn't reach their ends.
All inputs are finite; a program needn't handle non-finite values.
Results may differ from the reference program's by a relative error of at most 0.0066.
Values sent between devices are 32-bit elements; how exact they have to be, the bound alone decides.
A program may use at most 192 MiB of HBM per device.

```python
import math
import jax
import jax.numpy as jnp
from jax import lax

P_SIZE = 196
C = 1024
DS = 512
DC = 4096
IMG = 2
BATCH = 256


def spiked(drawn, stream_key, source, target, shards_of, factor):
    def block_of(position):
        return (jnp.arange(drawn.shape[position]) // (drawn.shape[position] // shards_of)).reshape((-1,) + (1,) * (drawn.ndim - 1 - position))

    one_side = jax.random.permutation(stream_key, shards_of)[block_of(target)]
    second = (block_of(target) + shards_of // 2) % shards_of
    return jnp.where((block_of(source) == one_side) | (block_of(source) == second), factor * drawn, drawn)


def levels(key, shape, cuts, least, largest):
    loudness, own = 1.0, jax.random.fold_in(key, 6)
    for position, blocks in cuts:
        heights = jnp.exp(jax.random.uniform(jax.random.fold_in(own, position), (blocks,), jnp.float32, least / len(cuts), largest / len(cuts)))
        loudness = loudness * jnp.repeat(heights, shape[position] // blocks).reshape([-1 if axis == position else 1 for axis in range(len(shape))])
    return loudness


def bell_draw(stream_key, dims, spread, bound, pieces=(), kind=jnp.bfloat16):
    array = spread * jax.random.normal(stream_key, dims, jnp.float32)
    if pieces:
        array = array * levels(stream_key, dims, pieces, -0.22, 0.18)
    return jnp.clip(array, -bound, bound).astype(kind)


def gaussian_with(rng, extent, width, bound, cuts, heavy, kind=jnp.bfloat16):
    array = width * jax.random.normal(rng, extent, jnp.float32)
    if cuts:
        array = array * levels(rng, extent, cuts, -0.22, 0.18)
    return jnp.clip(spiked(array, jax.random.fold_in(rng, 3), *heavy), -bound, bound).astype(kind)


def setup_inputs(seed: int = 0) -> dict:
    key_of = jax.random.split(jax.random.key(seed), 13)
    return {
        "inputs": bell_draw(key_of[0], (BATCH, P_SIZE, C), 1.0, 6.0, ((0, 128),)),
        "cotangent": gaussian_with(key_of[1], (BATCH, P_SIZE, C), 1.0, 24.0, ((0, 128),), (0, 2, 128, 5.5)),
        "first_gain": jnp.clip(jax.random.uniform(key_of[2], (C,), jnp.float32, 0.5, 1.5), 0.5, 1.5),
        "first_shift": bell_draw(key_of[3], (C,), 0.5, 3.0, (), jnp.float32),
        "token_in": bell_draw(key_of[4], (DS, P_SIZE), P_SIZE ** -0.5, 0.4375),
        "token_in_bias": bell_draw(key_of[5], (DS,), 0.5, 3.0, (), jnp.float32),
        "token_out": bell_draw(key_of[6], (DS, P_SIZE), DS ** -0.5, 0.25),
        "second_gain": jnp.clip(jax.random.uniform(key_of[7], (C,), jnp.float32, 0.5, 1.5), 0.5, 1.5),
        "second_shift": bell_draw(key_of[8], (C,), 0.5, 3.0, (), jnp.float32),
        "channel_in": bell_draw(key_of[9], (C, DC), C ** -0.5, 0.1875),
        "channel_in_bias": bell_draw(key_of[10], (DC,), 0.5, 3.0, (), jnp.float32),
        "channel_out": bell_draw(key_of[11], (C, DC), DC ** -0.5, 0.09375),
    }


epsilon = 1e-06

def norm_forward(values, gain, shift):
    centred = values - lax.optimization_barrier(jnp.mean(values, axis=-1, keepdims=True))
    variance = lax.optimization_barrier(jnp.mean(centred * centred, axis=-1, keepdims=True))
    inv_std = lax.rsqrt(variance + epsilon)
    scaled = centred * inv_std
    return (scaled * gain + shift, scaled, inv_std)

def norm_backward(incoming, scaled, inv_std, gain):
    weighted = incoming * gain
    first_mean = lax.optimization_barrier(jnp.mean(weighted, axis=-1, keepdims=True))
    second_mean = lax.optimization_barrier(jnp.mean(weighted * scaled, axis=-1, keepdims=True))
    return inv_std * (weighted - first_mean - scaled * second_mean)

def gelu_value(values):
    return 0.5 * values * (1.0 + lax.erf(values / math.sqrt(2.0)))

def gelu_slope(values):
    return 0.5 * (1.0 + lax.erf(values / math.sqrt(2.0))) + values * jnp.exp(-0.5 * values * values) / math.sqrt(2.0 * math.pi)

def reference(inputs, cotangent, first_gain, first_shift, token_in, token_in_bias, token_out, second_gain, second_shift, channel_in, channel_in_bias, channel_out):
    f32 = jnp.float32
    blocks = BATCH // IMG
    input_blocks = inputs.reshape(blocks, IMG, P_SIZE, C)
    cot_blocks = cotangent.reshape(blocks, IMG, P_SIZE, C)
    token_in_f = token_in.astype(f32)
    token_out_f = token_out.astype(f32)

    def one_block(carry, pair):
        x_block, g_block = pair
        x_float = x_block.astype(f32)
        g_float = g_block.astype(f32)
        normed_one, first_hat, first_rstd = norm_forward(x_float, first_gain, first_shift)
        normed1 = normed_one.astype(jnp.bfloat16)
        hidden1 = jnp.einsum('bpc,sp->bcs', normed1.astype(f32), token_in_f) + token_in_bias
        act1 = gelu_value(hidden1).astype(jnp.bfloat16)
        mixed = x_float + jnp.einsum('bcs,sp->bpc', act1.astype(f32), token_out_f)
        normed_two, second_hat, second_rstd = norm_forward(mixed, second_gain, second_shift)
        normed2 = normed_two.astype(jnp.bfloat16).reshape(-1, C)
        hidden2 = jnp.dot(normed2, channel_in, preferred_element_type=f32) + channel_in_bias
        act2 = gelu_value(hidden2).astype(jnp.bfloat16)
        cot_rows = g_block.reshape(-1, C)
        d_chout = jnp.dot(cot_rows.T, act2, preferred_element_type=f32)
        dact2 = jnp.dot(cot_rows, channel_out, preferred_element_type=f32)
        dhidden2 = (dact2 * gelu_slope(hidden2)).astype(jnp.bfloat16)
        d_chin = jnp.dot(normed2.T, dhidden2, preferred_element_type=f32)
        dnormed2 = jnp.dot(dhidden2, channel_in.T, preferred_element_type=f32).reshape(IMG, P_SIZE, C)
        dmixed = g_float + norm_backward(dnormed2, second_hat, second_rstd, second_gain)
        dmixed_round = dmixed.astype(jnp.bfloat16)
        d_tokout = jnp.einsum('bcs,bpc->sp', act1.astype(f32), dmixed_round.astype(f32))
        dact1 = jnp.einsum('bpc,sp->bcs', dmixed_round.astype(f32), token_out_f)
        dhidden1 = (dact1 * gelu_slope(hidden1)).astype(jnp.bfloat16)
        d_tokin = jnp.einsum('bcs,bpc->sp', dhidden1.astype(f32), normed1.astype(f32))
        dnormed1 = jnp.einsum('bcs,sp->bpc', dhidden1.astype(f32), token_in_f)
        grad_block = (dmixed + norm_backward(dnormed1, first_hat, first_rstd, first_gain)).astype(jnp.bfloat16)
        norms_part = jnp.stack([lax.optimization_barrier(jnp.sum(dnormed1 * first_hat, axis=(0, 1))), lax.optimization_barrier(jnp.sum(dnormed1, axis=(0, 1))), lax.optimization_barrier(jnp.sum(dnormed2 * second_hat, axis=(0, 1))), lax.optimization_barrier(jnp.sum(dnormed2, axis=(0, 1))), lax.optimization_barrier(jnp.sum(g_float, axis=(0, 1)))])
        tb_in = lax.optimization_barrier(jnp.sum(dhidden1.astype(f32), axis=(0, 1)))
        tb_out = lax.optimization_barrier(jnp.sum(dmixed, axis=(0, 2)))
        cb_in = lax.optimization_barrier(jnp.sum(dhidden2.astype(f32), axis=0))
        parts = (d_tokin, d_tokout, d_chin, d_chout, norms_part, tb_in, tb_out, cb_in)
        carry = tuple((a + b for a, b in zip(carry, parts)))
        return (carry, grad_block)
    start = (jnp.zeros((DS, P_SIZE), f32), jnp.zeros((DS, P_SIZE), f32), jnp.zeros((C, DC), f32), jnp.zeros((C, DC), f32), jnp.zeros((5, C), f32), jnp.zeros((DS,), f32), jnp.zeros((P_SIZE,), f32), jnp.zeros((DC,), f32))
    totals, grad_blocks = lax.scan(one_block, start, (input_blocks, cot_blocks))
    grad_inputs = grad_blocks.reshape(BATCH, P_SIZE, C)
    return (grad_inputs, totals[0], totals[1], totals[2], totals[3], totals[4], totals[5], totals[6], totals[7])
```

```python
import math

import jax
import jax.numpy as jnp
from jax import lax
from jax.experimental import pallas as pl
from jax.experimental.pallas import tpu as pltpu
from jax.sharding import Mesh
from jax.sharding import PartitionSpec as P

DEV = ("dev_0", "dev_1", "dev_2", "dev_3")
GRP_DEV = ("grp", "dev_0", "dev_1", "dev_2", "dev_3")
MESH = pl.DeviceIdType.MESH

epsilon = 1e-06

CHUNKS = 8
WIDTH = 512
ROWS = 400
COLOURS = (("x", "z", "y", 384), ("y", "z", "x", 384), ("z", "x", "y", 256))
FIRST = (0, 384, 768)
LAG = (0, 2, 5, 8, 11, 14, 17, 20)
SLOTS = CHUNKS + (LAG[-1] + 1) // 2


def remainder(a, b):
    return lax.rem(a, jnp.int32(b))


def where_on(fixed, half=None):
    index = [slice(None)] * 4
    for axis, at in fixed.items():
        if axis == "x":
            index[0] = at
        elif axis == "y":
            index[2] = at
        else:
            index[1] = remainder(at, 2)
            index[3] = lax.div(at, jnp.int32(2))
    if half is not None:
        axis, part = half
        if axis == "z_lo":
            index[1] = part
        else:
            index[0 if axis == "x" else 2] = pl.ds(2 * part, 2)
    return tuple(index)


HALVES = (("z_lo", "y"), ("z_lo", "x"), ("x", "y"))
HALF_SHAPES = (((4, 2), (2,)), ((4, 2), (2,)), ((2, 4), (2,)))
BLOCK_SHAPES = (((2, 4, 2), (4,)), ((4, 2, 2), (4,)), ((4, 4), (4,)))


def scratch_of():
    f32, bf16, dma = jnp.float32, jnp.bfloat16, pltpu.SemaphoreType.DMA
    shapes = {}
    for c, (_, _, _, width) in enumerate(COLOURS):
        shapes[f"own{c}"] = pltpu.VMEM((2, 4, 2, 4, 2, 2, 8, width), f32)
        shapes[f"sum{c}"] = pltpu.VMEM((CHUNKS, 4, 2, 4, 2, 8, width), f32)
        for p in range(2):
            shapes[f"half{c}{p}"] = pltpu.VMEM((CHUNKS, 2, *HALF_SHAPES[c][p], 8, width), f32)
            shapes[f"block{c}{p}"] = pltpu.VMEM((CHUNKS, 2, *BLOCK_SHAPES[c][p], 8, width), f32)
        shapes[f"last{c}"] = pltpu.VMEM((CHUNKS, 3, 8, width), f32)
    shapes["done"] = pltpu.VMEM((2, CHUNKS, 8, 2 * WIDTH), f32)
    shapes["w_in"] = pltpu.VMEM((2, 1024, WIDTH), bf16)
    shapes["w_out"] = pltpu.VMEM((2, 1024, WIDTH), bf16)
    shapes["act"] = pltpu.VMEM((512, WIDTH), bf16)
    shapes["dhid"] = pltpu.VMEM((512, WIDTH), bf16)
    shapes["hid"] = pltpu.VMEM((ROWS, WIDTH), f32)
    shapes["dact"] = pltpu.VMEM((ROWS, WIDTH), f32)
    shapes["w_sem"] = dma((2, 2))
    shapes["pair_send"] = dma((3,))
    shapes["pair_recv"] = dma((CHUNKS, 3))
    for p in range(2):
        shapes[f"half_send{p}"] = dma((3, 2))
        shapes[f"half_recv{p}"] = dma((CHUNKS, 3, 2))
        shapes[f"block_send{p}"] = dma((3, 2))
        shapes[f"block_recv{p}"] = dma((CHUNKS, 3, 2))
    shapes["last_send"] = dma((3, 3))
    shapes["last_recv"] = dma((CHUNKS, 3, 3))
    shapes["both_send"] = dma((1,))
    shapes["both_recv"] = dma((CHUNKS,))
    return shapes


def channel_kernel(names, n2, n2t, cot, cott, win, wout, bias, dn2, grads, cb, *scratch):
    r = dict(zip(names, scratch))
    f32, bf16 = jnp.float32, jnp.bfloat16
    x, y, core = lax.axis_index("dev_0"), lax.axis_index("dev_2"), lax.axis_index("dev_3")
    high = lax.axis_index("grp")
    me = {"x": x, "y": y, "z": 2 * high + lax.axis_index("dev_1")}

    def device(core=core, **moved):
        at = {**me, **moved}
        return (lax.div(at["z"], jnp.int32(2)), at["x"], remainder(at["z"], 2), at["y"], core)

    def along(axis, by):
        return remainder(me[axis] + by, 4)

    partners = [device(core=1 - core)]
    for axis in ("x", "y", "z"):
        partners += [device(**{axis: along(axis, by)}) for by in (1, 2, 3)]
    barrier = pltpu.get_barrier_semaphore()
    for partner in partners:
        pl.semaphore_signal(barrier, inc=1, device_id=partner, device_id_type=MESH)
    pl.semaphore_wait(barrier, len(partners))

    def remote(source, target, send, recv, to):
        return pltpu.make_async_remote_copy(
            src_ref=source, dst_ref=target, send_sem=send, recv_sem=recv, device_id=to, device_id_type=MESH
        )

    def fixed_before(c, p):
        return {axis: me[axis] for axis in COLOURS[c][:p]}

    def pair_copies(j):
        slot = remainder(j, 2)
        every = slice(None)
        return [
            remote(
                r[f"own{c}"].at[slot, every, every, every, 1 - core],
                r[f"sum{c}"].at[j],
                r["pair_send"].at[c],
                r["pair_recv"].at[j, c],
                device(core=1 - core),
            )
            for c in range(3)
        ]

    def half_copies(j, p):
        copies = []
        for c in range(3):
            axis = COLOURS[c][p]
            for d, by in enumerate((1, 3)):
                spot = where_on({**fixed_before(c, p), axis: along(axis, 2)}, (HALVES[c][p], d))
                copies.append(
                    remote(
                        r[f"sum{c}"].at[(j, *spot)],
                        r[f"half{c}{p}"].at[j, d],
                        r[f"half_send{p}"].at[c, d],
                        r[f"half_recv{p}"].at[j, c, d],
                        device(**{axis: along(axis, by)}),
                    )
                )
        return copies

    def block_copies(j, p):
        copies = []
        for c in range(3):
            axis = COLOURS[c][p]
            for d, by in enumerate((1, 3)):
                spot = where_on({**fixed_before(c, p), axis: along(axis, by)})
                copies.append(
                    remote(
                        r[f"sum{c}"].at[(j, *spot)],
                        r[f"block{c}{p}"].at[j, d],
                        r[f"block_send{p}"].at[c, d],
                        r[f"block_recv{p}"].at[j, c, d],
                        device(**{axis: along(axis, by)}),
                    )
                )
        return copies

    def last_copies(j):
        copies = []
        for c in range(3):
            axis = COLOURS[c][2]
            for d, by in enumerate((1, 2, 3)):
                spot = where_on({**fixed_before(c, 2), axis: along(axis, by)})
                copies.append(
                    remote(
                        r[f"sum{c}"].at[(j, *spot)],
                        r[f"last{c}"].at[j, d],
                        r["last_send"].at[c, d],
                        r["last_recv"].at[j, c, d],
                        device(**{axis: along(axis, by)}),
                    )
                )
        return copies

    def both_copy(j):
        return remote(
            r["done"].at[high, j],
            r["done"].at[high, j],
            r["both_send"].at[0],
            r["both_recv"].at[j],
            device(z=along("z", 2)),
        )

    def start(copies):
        for copy in copies:
            copy.start()

    def wait(copies):
        for copy in copies:
            copy.wait()

    def stage(s, j):
        if s == 1:
            wait(pair_copies(j))
            slot = remainder(j, 2)
            for c in range(3):
                for b in range(4):
                    r[f"sum{c}"][j, b] += r[f"own{c}"][slot, b, :, :, core]
            start(half_copies(j, 0))
        elif s in (2, 4):
            p = s // 2 - 1
            wait(half_copies(j, p))
            for c in range(3):
                axis = COLOURS[c][p]
                for d, by in enumerate((1, 3)):
                    spot = where_on({**fixed_before(c, p), axis: along(axis, by)}, (HALVES[c][p], d))
                    r[f"sum{c}"][(j, *spot)] += r[f"half{c}{p}"][j, d]
            start(block_copies(j, p))
        elif s in (3, 5):
            p = s // 2 - 1
            wait(block_copies(j, p))
            for c in range(3):
                spot = where_on(fixed_before(c, p + 1))
                r[f"sum{c}"][(j, *spot)] += r[f"block{c}{p}"][j, 0] + r[f"block{c}{p}"][j, 1]
            start(half_copies(j, 1) if p == 0 else last_copies(j))
        elif s == 6:
            wait(last_copies(j))
            for c in range(3):
                width = COLOURS[c][3]
                spot = where_on(me)
                got = r[f"last{c}"]
                r["done"][high, j, :, FIRST[c] : FIRST[c] + width] = (
                    r[f"sum{c}"][(j, *spot)] + got[j, 0] + (got[j, 1] + got[j, 2])
                )
            start([both_copy(j)])
        else:
            wait([both_copy(j)])

    def tick(t, parity):
        for s in range(7, 0, -1):
            if (LAG[s] - parity) % 2 == 0:
                j = t - (LAG[s] - parity) // 2

                @pl.when((j >= 0) & (j < CHUNKS))
                def _():
                    stage(s, j)

    def weights(j):
        slot = remainder(j, 2)
        columns = pl.ds(pl.multiple_of(j * WIDTH, WIDTH), WIDTH)
        return [
            pltpu.make_async_copy(win.at[:, columns], r["w_in"].at[slot], r["w_sem"].at[slot, 0]),
            pltpu.make_async_copy(wout.at[:, columns], r["w_out"].at[slot], r["w_sem"].at[slot, 1]),
        ]

    act, dhid, hid, dact = r["act"], r["dhid"], r["hid"], r["dact"]

    def forward(j):
        slot = remainder(j, 2)
        wait(weights(j))

        @pl.when(j + 1 < CHUNKS)
        def _():
            start(weights(j + 1))

        columns = pl.ds(pl.multiple_of(j * WIDTH, WIDTH), WIDTH)
        for b in range(WIDTH // 256):
            part = slice(256 * b, 256 * (b + 1))
            hid[:, part] = jnp.dot(n2[...], r["w_in"][slot, :, part], preferred_element_type=f32)
            dact[:, part] = jnp.dot(cot[...], r["w_out"][slot, :, part], preferred_element_type=f32)
        shift = bias[:, columns]

        def rows(i, total):
            at = pl.ds(pl.multiple_of(i * 80, 80), 80)
            v = hid[at, :] + shift
            twice = 1.0 + lax.erf(v * (1.0 / math.sqrt(2.0)))
            act[at, :] = (0.5 * v * twice).astype(bf16)
            slope = 0.5 * twice + v * jnp.exp(-0.5 * v * v) * (1.0 / math.sqrt(2.0 * math.pi))
            d = (dact[at, :] * slope).astype(bf16)
            dhid[at, :] = d
            return total + jnp.sum(d.astype(f32).reshape(10, 8, WIDTH), axis=0)

        total = lax.fori_loop(0, ROWS // 80, rows, jnp.zeros((8, WIDTH), f32))
        cb[:, columns] = jnp.sum(total, axis=0, keepdims=True)

    def gradients(j):
        slot = remainder(j, 2)

        def rows(i, _):
            at = pl.ds(pl.multiple_of(i * 256, 256), 256)
            out = jnp.dot(cott[at, :], act[...], preferred_element_type=f32).reshape(2, 4, 2, 2, 8, WIDTH)
            r["own0"][slot, i] = out[..., :384]
            r["own1"][slot, i, :, :, :, :, :, :128] = out[..., 384:]
            inn = jnp.dot(n2t[at, :], dhid[...], preferred_element_type=f32).reshape(2, 4, 2, 2, 8, WIDTH)
            r["own1"][slot, i, :, :, :, :, :, 128:] = inn[..., :256]
            r["own2"][slot, i] = inn[..., 256:]
            return 0

        lax.fori_loop(0, 4, rows, 0)
        start(pair_copies(j))
        for b in range(4):
            part = slice(256 * b, 256 * (b + 1))
            dn2[:, part] += lax.dot_general(
                dhid[:ROWS, :],
                r["w_in"][slot, part, :],
                (((1,), (1,)), ((), ())),
                preferred_element_type=f32,
            )

    start(weights(jnp.int32(0)))
    act[ROWS:, :] = jnp.zeros((512 - ROWS, WIDTH), bf16)
    dhid[ROWS:, :] = jnp.zeros((512 - ROWS, WIDTH), bf16)
    dn2[...] = jnp.zeros_like(dn2)

    def slot_of(t, _):
        @pl.when(t < CHUNKS)
        def _():
            forward(t)

        tick(t, 0)

        @pl.when(t < CHUNKS)
        def _():
            gradients(t)

        tick(t, 1)
        return 0

    lax.fori_loop(0, SLOTS, slot_of, 0)
    for h in range(2):
        for j in range(CHUNKS):
            for g in range(2):
                grads[g, 8 * h : 8 * (h + 1), WIDTH * j : WIDTH * (j + 1)] = r["done"][
                    h, j, :, WIDTH * g : WIDTH * (g + 1)
                ]


def channel_stage(normed2, cot_rows, channel_in, channel_out, channel_in_bias):
    f32 = jnp.float32
    tokens, channels = normed2.shape
    hidden = channel_in.shape[1]
    down = lambda a: jnp.pad(a, ((0, ROWS - tokens), (0, 0)))
    across = lambda a: jnp.pad(a.T, ((0, 0), (0, 512 - tokens)))
    shapes = scratch_of()
    vmem, anywhere = pl.BlockSpec(memory_space=pltpu.VMEM), pl.BlockSpec(memory_space=pl.ANY)
    names = tuple(shapes)

    def kernel(*refs):
        channel_kernel(names, *refs)

    dn2, grads, cb = pl.pallas_call(
        kernel,
        out_shape=(
            jax.ShapeDtypeStruct((ROWS, channels), f32),
            jax.ShapeDtypeStruct((2, 16, hidden), f32),
            jax.ShapeDtypeStruct((1, hidden), f32),
        ),
        in_specs=[vmem, vmem, vmem, vmem, anywhere, anywhere, vmem],
        out_specs=(vmem, vmem, vmem),
        scratch_shapes=list(shapes.values()),
        compiler_params=pltpu.CompilerParams(collective_id=0, has_side_effects=True, vmem_limit_bytes=66_000_000),
        name="channel_stage",
    )(
        down(normed2),
        across(normed2),
        down(cot_rows),
        across(cot_rows),
        channel_in,
        channel_out,
        channel_in_bias.reshape(1, -1),
    )
    return dn2[:tokens], grads[0], grads[1], cb[0]


def cut_along(shard, dim, count):
    before, after = (shard.shape[:dim], shard.shape[dim + 1 :])
    return jnp.moveaxis(shard.reshape(*before, count, -1, *after), dim, 0)


def summed_on_arrival(shard, axis, dim):
    count = lax.axis_size(axis)
    blocks = lax.all_to_all(cut_along(shard, dim, count), axis, 0, 0, tiled=True)
    return jnp.sum(blocks, axis=0)


def copy_for_each(shard, axis):
    copies = jnp.broadcast_to(shard, (lax.axis_size(axis), *shard.shape))
    return lax.all_to_all(copies, axis, split_axis=0, concat_axis=0, tiled=True)


def of_everyone(shard, axis):
    everything = copy_for_each(shard, axis)
    return jnp.sum(everything, axis=0)


def together(arrays, axis):
    line, at, gathered = (jnp.concatenate([a.reshape(-1) for a in arrays]), 0, [])
    running = of_everyone(line, axis)
    for a in arrays:
        gathered.append(running[at : at + a.size].reshape(a.shape))
        at += a.size
    return tuple(gathered)


def together_2(arrays, axis):
    ends = [0]
    for a in arrays:
        ends.append(ends[-1] + a.size)
    running = lax.psum(jnp.concatenate([a.ravel() for a in arrays]), axis)
    return tuple((running[b:e].reshape(a.shape) for a, b, e in zip(arrays, ends, ends[1:])))


def norm_forward(values, gain, shift):
    centred = values - jnp.mean(values, axis=-1, keepdims=True)
    variance = jnp.mean(centred * centred, axis=-1, keepdims=True)
    inv_std = lax.rsqrt(variance + epsilon)
    scaled = centred * inv_std
    return (scaled * gain + shift, scaled, inv_std)


def norm_backward(incoming, scaled, inv_std, gain):
    weighted = incoming * gain
    first_mean = jnp.mean(weighted, axis=-1, keepdims=True)
    second_mean = jnp.mean(weighted * scaled, axis=-1, keepdims=True)
    return inv_std * (weighted - first_mean - scaled * second_mean)


def gelu_value(values):
    return 0.5 * values * (1.0 + lax.erf(values / math.sqrt(2.0)))


def gelu_slope(values):
    return 0.5 * (1.0 + lax.erf(values / math.sqrt(2.0))) + values * jnp.exp(
        -0.5 * values * values
    ) / math.sqrt(2.0 * math.pi)


def per_device(
    inputs,
    cotangent,
    first_gain,
    first_shift,
    token_in,
    token_in_bias,
    token_out,
    second_gain,
    second_shift,
    channel_in,
    channel_in_bias,
    channel_out,
):
    f32 = jnp.float32
    images, patches, channels = inputs.shape
    x_float = inputs.astype(f32)
    g_float = cotangent.astype(f32)
    normed_one, first_hat, first_rstd = norm_forward(x_float, first_gain, first_shift)
    normed1 = normed_one.astype(jnp.bfloat16)
    hidden1 = (
        jnp.einsum("bpc,sp->bcs", normed1, token_in, preferred_element_type=f32) + token_in_bias
    )
    act1 = gelu_value(hidden1).astype(jnp.bfloat16)
    mixed = x_float + jnp.einsum("bcs,sp->bpc", act1, token_out, preferred_element_type=f32)
    normed_two, second_hat, second_rstd = norm_forward(mixed, second_gain, second_shift)
    normed2 = normed_two.astype(jnp.bfloat16).reshape(-1, channels)
    cot_rows = cotangent.reshape(-1, channels)
    dnormed2, chout_part, chin_part, cb_in = channel_stage(
        normed2, cot_rows, channel_in, channel_out, channel_in_bias
    )
    dnormed2 = dnormed2.reshape(images, patches, channels)
    dmixed = g_float + norm_backward(dnormed2, second_hat, second_rstd, second_gain)
    dmixed_round = dmixed.astype(jnp.bfloat16)
    dact1 = jnp.einsum("bpc,sp->bcs", dmixed_round, token_out, preferred_element_type=f32)
    dhidden1 = (dact1 * gelu_slope(hidden1)).astype(jnp.bfloat16)
    dnormed1 = jnp.einsum("bcs,sp->bpc", dhidden1, token_in, preferred_element_type=f32)
    grad_inputs = (dmixed + norm_backward(dnormed1, first_hat, first_rstd, first_gain)).astype(
        jnp.bfloat16
    )
    grad_in_piece = jnp.einsum("bcs,bpc->sp", dhidden1, normed1, preferred_element_type=f32)
    grad_out_piece = jnp.einsum("bcs,bpc->sp", act1, dmixed_round, preferred_element_type=f32)
    token_part = summed_on_arrival(jnp.concatenate([grad_in_piece, grad_out_piece], axis=1), DEV, 0)
    (token_part,) = together((token_part,), "grp")
    norms_part = jnp.stack(
        [
            jnp.sum(dnormed1 * first_hat, axis=(0, 1)),
            jnp.sum(dnormed1, axis=(0, 1)),
            jnp.sum(dnormed2 * second_hat, axis=(0, 1)),
            jnp.sum(dnormed2, axis=(0, 1)),
            jnp.sum(g_float, axis=(0, 1)),
        ]
    )
    tb_in = jnp.sum(dhidden1.astype(f32), axis=(0, 1))
    tb_out = jnp.sum(dmixed, axis=(0, 2))
    norms_total, tb_in_total, tb_out_total, cb_in_total = together_2(
        (norms_part, tb_in, tb_out, cb_in), GRP_DEV
    )
    return (
        grad_inputs,
        token_part[:, :patches],
        token_part[:, patches:],
        chin_part,
        chout_part,
        norms_total,
        tb_in_total,
        tb_out_total,
        cb_in_total,
    )


def solution(mesh):
    split = Mesh(
        mesh.devices.reshape(mesh.shape["grp"], 4, 2, 4, 2),
        ("grp", "dev_0", "dev_1", "dev_2", "dev_3"),
    )
    in_specs = (
        P(GRP_DEV, None, None),
        P(GRP_DEV, None, None),
        P(),
        P(),
        P(),
        P(),
        P(),
        P(),
        P(),
        P(),
        P(),
        P(),
    )
    out_specs = (
        P(GRP_DEV, None, None),
        P(DEV, None),
        P(DEV, None),
        P(DEV, None),
        P(DEV, None),
        P(),
        P(),
        P(),
        P(),
    )
    return jax.shard_map(
        per_device, mesh=split, in_specs=in_specs, out_specs=out_specs, check_vma=False
    )
```

```python
import math

import jax
import jax.numpy as jnp
from jax import lax
from jax.experimental import pallas as pl
from jax.experimental.pallas import tpu as pltpu
from jax.sharding import Mesh
from jax.sharding import PartitionSpec as P

DEV = ("dev_0", "dev_1", "dev_2", "dev_3")
GRP_DEV = ("grp", "dev_0", "dev_1", "dev_2", "dev_3")
MESH = pl.DeviceIdType.MESH

epsilon = 1e-06

CHUNKS = 8
WIDTH = 512
IMAGE = 208
ROWS = 416
PATCHES = 196
RING = 4
COLOURS = (("x", "z", "y", 384), ("y", "z", "x", 384), ("z", "x", "y", 256))
FIRST = (0, 384, 768)
LAG = (0, 2, 5, 8, 11, 14, 17, 20)
LATE = CHUNKS + 2
SLOTS = LATE + (LAG[-1] + 2) // 2


def remainder(a, b):
    return lax.rem(a, jnp.int32(b))


def where_on(fixed, half=None):
    index = [slice(None)] * 4
    for axis, at in fixed.items():
        if axis == "x":
            index[0] = at
        elif axis == "y":
            index[2] = at
        else:
            index[1] = remainder(at, 2)
            index[3] = lax.div(at, jnp.int32(2))
    if half is not None:
        axis, part = half
        if axis == "z_lo":
            index[1] = part
        else:
            index[0 if axis == "x" else 2] = pl.ds(2 * part, 2)
    return tuple(index)


HALVES = (("z_lo", "y"), ("z_lo", "x"), ("x", "y"))
HALF_SHAPES = (((4, 2), (2,)), ((4, 2), (2,)), ((2, 4), (2,)))
BLOCK_SHAPES = (((2, 4, 2), (4,)), ((4, 2, 2), (4,)), ((4, 4), (4,)))


def gelu_parts(v):
    twice = 1.0 + lax.erf(v * (1.0 / math.sqrt(2.0)))
    value = 0.5 * v * twice
    slope = 0.5 * twice + v * jnp.exp(-0.5 * v * v) * (1.0 / math.sqrt(2.0 * math.pi))
    return value, slope


def standardized(values):
    centred = values - jnp.mean(values, axis=-1, keepdims=True)
    rstd = lax.rsqrt(jnp.mean(centred * centred, axis=-1, keepdims=True) + epsilon)
    return centred * rstd, rstd


def norm_backward(incoming, scaled, inv_std, gain):
    weighted = incoming * gain
    first_mean = jnp.mean(weighted, axis=-1, keepdims=True)
    second_mean = jnp.mean(weighted * scaled, axis=-1, keepdims=True)
    return inv_std * (weighted - first_mean - scaled * second_mean)


def scratch_of():
    f32, bf16, dma = jnp.float32, jnp.bfloat16, pltpu.SemaphoreType.DMA
    shapes = {}
    for c, (_, _, _, width) in enumerate(COLOURS):
        chunks = CHUNKS + 1 if c == 2 else CHUNKS
        shapes[f"own{c}"] = pltpu.VMEM((4, 2, 4, 2, 2, 8, width), f32)
        shapes[f"sum{c}"] = pltpu.VMEM((chunks, 4, 2, 4, 2, 8, width), f32)
        for p in range(2):
            kept = RING if p == 0 else chunks
            shapes[f"half{c}{p}"] = pltpu.VMEM((kept, 2, *HALF_SHAPES[c][p], 8, width), f32)
            shapes[f"block{c}{p}"] = pltpu.VMEM((kept, 2, *BLOCK_SHAPES[c][p], 8, width), f32)
        shapes[f"last{c}"] = pltpu.VMEM((chunks, 3, 8, width), f32)
    shapes["done"] = pltpu.VMEM((2, CHUNKS, 8, 2 * WIDTH), f32)
    shapes["done_token"] = pltpu.VMEM((2, 8, 256), f32)
    shapes["w_in"] = pltpu.VMEM((2, 1024, WIDTH), bf16)
    shapes["w_out"] = pltpu.VMEM((2, 1024, WIDTH), bf16)
    shapes["act"] = pltpu.VMEM((512, WIDTH), bf16)
    shapes["dhid"] = pltpu.VMEM((512, WIDTH), bf16)
    shapes["hid"] = pltpu.VMEM((512, WIDTH), f32)
    shapes["dact"] = pltpu.VMEM((512, WIDTH), f32)
    shapes["xs"] = pltpu.VMEM((2, IMAGE, 1024), bf16)
    shapes["n1"] = pltpu.VMEM((2, 256, 1024), bf16)
    shapes["act1"] = pltpu.VMEM((2, 512, 1024), bf16)
    shapes["hat2"] = pltpu.VMEM((ROWS, 1024), f32)
    shapes["rstd2"] = pltpu.VMEM((ROWS, 128), f32)
    shapes["n2"] = pltpu.VMEM((512, 1024), bf16)
    shapes["n2t"] = pltpu.VMEM((1024, 512), bf16)
    shapes["cots"] = pltpu.VMEM((512, 1024), bf16)
    shapes["cott"] = pltpu.VMEM((1024, 512), bf16)
    for name in ("tin", "tout"):
        shapes[name] = pltpu.VMEM((512, 256), bf16)
        shapes[name + "t"] = pltpu.VMEM((256, 512), bf16)
        shapes["grad_" + name] = pltpu.VMEM((512, 256), f32)
    shapes["dmr"] = pltpu.VMEM((2, 256, 1024), bf16)
    shapes["dh1"] = pltpu.VMEM((2, 512, 1024), bf16)
    shapes["dn2"] = pltpu.VMEM((ROWS, 1024), f32)
    shapes["columns"] = pltpu.VMEM((256, 128), f32)
    shapes["vector"] = pltpu.VMEM((16, 1024), f32)
    shapes["vector_pair"] = pltpu.VMEM((16, 1024), f32)
    for axis in "xyz":
        shapes["vector_" + axis] = pltpu.VMEM((4, 16, 1024), f32)
    shapes["vector_send"] = dma((3,))
    shapes["vector_recv"] = dma((4, 3))
    shapes["w_sem"] = dma((2, 2))
    shapes["pair_send"] = dma((3,))
    shapes["pair_recv"] = dma((CHUNKS + 1, 3))
    for p in range(2):
        shapes[f"half_send{p}"] = dma((3, 2))
        shapes[f"half_recv{p}"] = dma((CHUNKS + 1, 3, 2))
        shapes[f"block_send{p}"] = dma((3, 2))
        shapes[f"block_recv{p}"] = dma((CHUNKS + 1, 3, 2))
    shapes["last_send"] = dma((3, 3))
    shapes["last_recv"] = dma((CHUNKS + 1, 3, 3))
    shapes["both_send"] = dma((1,))
    shapes["both_recv"] = dma((CHUNKS + 1,))
    return shapes


def block_kernel(names, *refs):
    inputs, cotangent, gain1, shift1, token_in, bias1, token_out, gain2, shift2, win, bias2, wout = refs[:12]
    grad_inputs, grad_tin, grad_tout, grad_in, grad_out, grad_norms, grad_b1, grad_bo, grad_b2 = refs[12:21]
    r = dict(zip(names, refs[21:]))
    f32, bf16 = jnp.float32, jnp.bfloat16
    x, y, core = lax.axis_index("dev_0"), lax.axis_index("dev_2"), lax.axis_index("dev_3")
    high = lax.axis_index("grp")
    me = {"x": x, "y": y, "z": 2 * high + lax.axis_index("dev_1")}

    def device(core=core, **moved):
        at = {**me, **moved}
        return (lax.div(at["z"], jnp.int32(2)), at["x"], remainder(at["z"], 2), at["y"], core)

    def along(axis, by):
        return remainder(me[axis] + by, 4)

    partners = [device(core=1 - core)]
    for axis in ("x", "y", "z"):
        partners += [device(**{axis: along(axis, by)}) for by in (1, 2, 3)]
    barrier = pltpu.get_barrier_semaphore()
    for partner in partners:
        pl.semaphore_signal(barrier, inc=1, device_id=partner, device_id_type=MESH)

    def remote(source, target, send, recv, to):
        return pltpu.make_async_remote_copy(
            src_ref=source, dst_ref=target, send_sem=send, recv_sem=recv, device_id=to, device_id_type=MESH
        )

    def fixed_before(c, p):
        return {axis: me[axis] for axis in COLOURS[c][:p]}

    def colours(j):
        return (2,) if isinstance(j, int) else (0, 1, 2)

    def kept(j, p):
        return remainder(j, RING) if p == 0 else j

    def pair_copies(j):
        every = slice(None)
        return [
            remote(
                r[f"own{c}"].at[every, every, every, 1 - core],
                r[f"sum{c}"].at[j],
                r["pair_send"].at[c],
                r["pair_recv"].at[j, c],
                device(core=1 - core),
            )
            for c in colours(j)
        ]

    def half_copies(j, p):
        copies = []
        for c in colours(j):
            axis = COLOURS[c][p]
            for d, by in enumerate((1, 3)):
                spot = where_on({**fixed_before(c, p), axis: along(axis, 2)}, (HALVES[c][p], d))
                copies.append(
                    remote(
                        r[f"sum{c}"].at[(j, *spot)],
                        r[f"half{c}{p}"].at[kept(j, p), d],
                        r[f"half_send{p}"].at[c, d],
                        r[f"half_recv{p}"].at[j, c, d],
                        device(**{axis: along(axis, by)}),
                    )
                )
        return copies

    def block_copies(j, p):
        copies = []
        for c in colours(j):
            axis = COLOURS[c][p]
            for d, by in enumerate((1, 3)):
                spot = where_on({**fixed_before(c, p), axis: along(axis, by)})
                copies.append(
                    remote(
                        r[f"sum{c}"].at[(j, *spot)],
                        r[f"block{c}{p}"].at[kept(j, p), d],
                        r[f"block_send{p}"].at[c, d],
                        r[f"block_recv{p}"].at[j, c, d],
                        device(**{axis: along(axis, by)}),
                    )
                )
        return copies

    def last_copies(j):
        copies = []
        for c in colours(j):
            axis = COLOURS[c][2]
            for d, by in enumerate((1, 2, 3)):
                spot = where_on({**fixed_before(c, 2), axis: along(axis, by)})
                copies.append(
                    remote(
                        r[f"sum{c}"].at[(j, *spot)],
                        r[f"last{c}"].at[j, d],
                        r["last_send"].at[c, d],
                        r["last_recv"].at[j, c, d],
                        device(**{axis: along(axis, by)}),
                    )
                )
        return copies

    def both_copy(j):
        mine = r["done_token"].at[high] if isinstance(j, int) else r["done"].at[high, j]
        return remote(
            mine,
            mine,
            r["both_send"].at[0],
            r["both_recv"].at[j],
            device(z=along("z", 2)),
        )

    def start(copies):
        for copy in copies:
            copy.start()

    def wait(copies):
        for copy in copies:
            copy.wait()

    def stage(s, j):
        if s == 1:
            wait(pair_copies(j))
            for c in colours(j):
                for b in range(4):
                    r[f"sum{c}"][j, b] += r[f"own{c}"][b, :, :, core]
            start(half_copies(j, 0))
        elif s in (2, 4):
            p = s // 2 - 1
            wait(half_copies(j, p))
            for c in colours(j):
                axis = COLOURS[c][p]
                for d, by in enumerate((1, 3)):
                    spot = where_on({**fixed_before(c, p), axis: along(axis, by)}, (HALVES[c][p], d))
                    r[f"sum{c}"][(j, *spot)] += r[f"half{c}{p}"][kept(j, p), d]
            start(block_copies(j, p))
        elif s in (3, 5):
            p = s // 2 - 1
            wait(block_copies(j, p))
            for c in colours(j):
                spot = where_on(fixed_before(c, p + 1))
                r[f"sum{c}"][(j, *spot)] += r[f"block{c}{p}"][kept(j, p), 0] + r[f"block{c}{p}"][kept(j, p), 1]
            start(half_copies(j, 1) if p == 0 else last_copies(j))
        elif s == 6:
            wait(last_copies(j))
            for c in colours(j):
                width = COLOURS[c][3]
                spot = where_on(me)
                got = r[f"last{c}"]
                total = r[f"sum{c}"][(j, *spot)] + got[j, 0] + (got[j, 1] + got[j, 2])
                if isinstance(j, int):
                    r["done_token"][high] = total
                else:
                    r["done"][high, j, :, FIRST[c] : FIRST[c] + width] = total
            start([both_copy(j)])
        else:
            wait([both_copy(j)])

    def tick(t, parity):
        for s in range(7, 0, -1):
            if (LAG[s] - parity) % 2 == 0:
                j = t - (LAG[s] - parity) // 2

                @pl.when((j >= 0) & (j < CHUNKS))
                def _():
                    stage(s, j)

                @pl.when(j == LATE)
                def _():
                    stage(s, CHUNKS)

    def weights(j):
        slot = remainder(j, 2)
        columns = pl.ds(pl.multiple_of(j * WIDTH, WIDTH), WIDTH)
        return [
            pltpu.make_async_copy(win.at[:, columns], r["w_in"].at[slot], r["w_sem"].at[slot, 0]),
            pltpu.make_async_copy(wout.at[:, columns], r["w_out"].at[slot], r["w_sem"].at[slot, 1]),
        ]

    act, dhid, hid, dact, dn2, vector = r["act"], r["dhid"], r["hid"], r["dact"], r["dn2"], r["vector"]

    def blocks_of(count, size, step, start_with=0):
        def at_block(i, carry):
            return step(pl.ds(pl.multiple_of(i * size, size), size), i, carry)

        return lax.fori_loop(0, count, at_block, start_with)

    def real(i):
        return lax.broadcasted_iota(jnp.int32, (16, 1), 0) + 16 * i < PATCHES

    def folded(values):
        return jnp.sum(values.reshape(2, 8, 1024), axis=0)

    def token_hidden(b, columns):
        hid[...] = jnp.dot(r["tin"][...], r["n1"][b, :, columns], preferred_element_type=f32)

    def prologue():
        for name, ref in (("tin", token_in), ("tout", token_out)):
            r[name][...] = jnp.zeros((512, 256), bf16)
            r[name][:, :PATCHES] = ref[...]
            r[name + "t"][...] = r[name][...].T
        for b in range(2):
            tail = jnp.zeros((256 - IMAGE, 1024), bf16)
            r["xs"][b, 192:, :] = jnp.zeros((16, 1024), bf16)
            r["xs"][b, :PATCHES, :] = inputs[b]
            r["cots"][IMAGE * b + 192 : IMAGE * b + 208, :] = jnp.zeros((16, 1024), bf16)
            r["cots"][IMAGE * b : IMAGE * b + PATCHES, :] = cotangent[b]
            r["n1"][b, IMAGE:, :] = tail
            r["dmr"][b, IMAGE:, :] = tail

            def first_norm(at, i, _):
                hat, _rstd = standardized(r["xs"][b, at, :].astype(f32))
                value = hat * gain1[...] + shift1[...]
                r["n1"][b, at, :] = jnp.where(real(i), value, 0.0).astype(bf16)
                return 0

            blocks_of(IMAGE // 16, 16, first_norm)
        r["cots"][ROWS:, :] = jnp.zeros((512 - ROWS, 1024), bf16)
        r["n2"][ROWS:, :] = jnp.zeros((512 - ROWS, 1024), bf16)
        r["cott"][...] = r["cots"][...].T
        for b in range(2):
            for half in range(2):
                columns = slice(512 * half, 512 * (half + 1))
                token_hidden(b, columns)

                def activate(at, i, _):
                    value = gelu_parts(hid[at, :] + bias1[at, :])[0]
                    r["act1"][b, at, columns] = value.astype(bf16)
                    return 0

                blocks_of(16, 32, activate)
            for q in range(4):
                columns = slice(256 * q, 256 * (q + 1))
                r["hat2"][IMAGE * b : IMAGE * (b + 1), columns] = jnp.dot(
                    r["toutt"][:IMAGE, :], r["act1"][b, :, columns], preferred_element_type=f32
                )

            def second_norm(at, i, _):
                rows = pl.ds(pl.multiple_of(IMAGE * b + 16 * i, 16), 16)
                hat, rstd = standardized(r["xs"][b, at, :].astype(f32) + r["hat2"][rows, :])
                r["hat2"][rows, :] = hat
                r["rstd2"][rows, :] = jnp.broadcast_to(rstd, (16, 128))
                value = hat * gain2[...] + shift2[...]
                r["n2"][rows, :] = jnp.where(real(i), value, 0.0).astype(bf16)
                return 0

            blocks_of(IMAGE // 16, 16, second_norm)
        r["n2t"][...] = r["n2"][...].T

    def forward(j):
        slot = remainder(j, 2)
        wait(weights(j))

        @pl.when(j + 1 < CHUNKS)
        def _():
            start(weights(j + 1))

        columns = pl.ds(pl.multiple_of(j * WIDTH, WIDTH), WIDTH)
        for b in range(WIDTH // 256):
            part = slice(256 * b, 256 * (b + 1))
            hid[:ROWS, part] = jnp.dot(r["n2"][:ROWS, :], r["w_in"][slot, :, part], preferred_element_type=f32)
            dact[:ROWS, part] = jnp.dot(r["cots"][:ROWS, :], r["w_out"][slot, :, part], preferred_element_type=f32)
        shift = bias2[:, columns]

        def rows(at, i, total):
            value, slope = gelu_parts(hid[at, :] + shift)
            act[at, :] = value.astype(bf16)
            d = (dact[at, :] * slope).astype(bf16)
            dhid[at, :] = d
            return total + jnp.sum(d.astype(f32).reshape(4, 8, WIDTH), axis=0)

        total = blocks_of(ROWS // 32, 32, rows, jnp.zeros((8, WIDTH), f32))
        half = pl.ds(pl.multiple_of(remainder(j, 2) * WIDTH, WIDTH), WIDTH)
        vector[pl.ds(5 + lax.div(j, jnp.int32(2)), 1), half] = jnp.sum(total, axis=0, keepdims=True)

    def gradients(j):
        slot = remainder(j, 2)

        def rows(at, i, _):
            out = jnp.dot(r["cott"][at, :], act[...], preferred_element_type=f32).reshape(2, 4, 2, 2, 8, WIDTH)
            r["own0"][i] = out[..., :384]
            r["own1"][i, :, :, :, :, :, :128] = out[..., 384:]
            inn = jnp.dot(r["n2t"][at, :], dhid[...], preferred_element_type=f32).reshape(2, 4, 2, 2, 8, WIDTH)
            r["own1"][i, :, :, :, :, :, 128:] = inn[..., :256]
            r["own2"][i] = inn[..., 256:]
            return 0

        blocks_of(4, 256, rows)
        start(pair_copies(j))
        for b in range(4):
            part = slice(256 * b, 256 * (b + 1))
            dn2[:, part] += lax.dot_general(
                dhid[:ROWS, :],
                r["w_in"][slot, part, :],
                (((1,), (1,)), ((), ())),
                preferred_element_type=f32,
            )

    def across(a, b):
        return lax.dot_general(a, b, (((1,), (1,)), ((), ())), preferred_element_type=f32)

    def token_backward(b):
        def second_norm(at, i, sums):
            rows = pl.ds(pl.multiple_of(IMAGE * b + 16 * i, 16), 16)
            hat, incoming = r["hat2"][rows, :], dn2[rows, :]
            g = r["cots"][rows, :].astype(f32)
            dmixed = g + norm_backward(incoming, hat, r["rstd2"][rows, :1], gain2[...])
            dn2[rows, :] = dmixed
            r["dmr"][b, at, :] = dmixed.astype(bf16)
            r["columns"][at, :] += jnp.broadcast_to(jnp.sum(dmixed, axis=1, keepdims=True), (16, 128))
            return (sums[0] + folded(incoming * hat), sums[1] + folded(incoming), sums[2] + folded(g))

        zero = jnp.zeros((8, 1024), f32)
        sums = blocks_of(IMAGE // 16, 16, second_norm, (zero, zero, zero))
        for row, total in zip((2, 3, 4), sums):
            vector[row : row + 1, :] += jnp.sum(total, axis=0, keepdims=True)
        for half in range(2):
            columns = slice(512 * half, 512 * (half + 1))
            token_hidden(b, columns)
            dact[...] = jnp.dot(r["tout"][...], r["dmr"][b, :, columns], preferred_element_type=f32)

            def back(at, i, _):
                slope = gelu_parts(hid[at, :] + bias1[at, :])[1]
                r["dh1"][b, at, columns] = (dact[at, :] * slope).astype(bf16)
                return 0

            blocks_of(16, 32, back)

    def token_gradients(b):
        r["grad_tin"][...] += across(r["dh1"][b], r["n1"][b])
        r["grad_tout"][...] += across(r["act1"][b], r["dmr"][b])
        ones = jnp.ones((8, 1024), bf16)
        vector[9:10, :512] += across(ones, r["dh1"][b])[:1]

    def send_token_gradients():
        for h, name in enumerate(("grad_tin", "grad_tout")):
            r["own2"][:, :, :, :, h] = r[name][...].reshape(4, 2, 4, 2, 8, 256)
        start(pair_copies(CHUNKS))

    def input_gradients(b):
        for half in range(2):
            columns = slice(512 * half, 512 * (half + 1))
            hid[:IMAGE, :] = jnp.dot(r["tint"][:IMAGE, :], r["dh1"][b, :, columns], preferred_element_type=f32)
            r["hat2"][:IMAGE, columns] = hid[:IMAGE, :]

        def first_norm(at, i, sums):
            hat, rstd = standardized(r["xs"][b, at, :].astype(f32))
            incoming = r["hat2"][at, :]
            rows = pl.ds(pl.multiple_of(IMAGE * b + 16 * i, 16), 16)
            total = dn2[rows, :] + norm_backward(incoming, hat, rstd, gain1[...])
            r["xs"][b, at, :] = total.astype(bf16)
            return (sums[0] + folded(incoming * hat), sums[1] + folded(incoming))

        zero = jnp.zeros((8, 1024), f32)
        sums = blocks_of(IMAGE // 16, 16, first_norm, (zero, zero))
        for row, total in zip((0, 1), sums):
            vector[row : row + 1, :] += jnp.sum(total, axis=0, keepdims=True)

    def vector_copies(step):
        if step == 0:
            return [
                remote(
                    vector, r["vector_pair"], r["vector_send"].at[0], r["vector_recv"].at[0, 0], device(core=1 - core)
                )
            ]
        axis = "xyz"[step - 1]
        at = r["vector_" + axis]
        return [
            remote(
                at.at[0],
                at.at[by],
                r["vector_send"].at[by - 1],
                r["vector_recv"].at[step, by - 1],
                device(**{axis: along(axis, by)}),
            )
            for by in (1, 2, 3)
        ]

    def vector_total(axis):
        at = r["vector_" + axis]
        terms = [at[remainder(me[axis] + 4 - k, 4)] for k in range(4)]
        return (terms[0] + terms[1]) + (terms[2] + terms[3])

    def vector_stage(step):
        if step == 0:
            vector[9:10, 512:768] = r["columns"][...].T[:1, :]
            start(vector_copies(0))
            return
        wait(vector_copies(step - 1))
        total = vector[...] + r["vector_pair"][...] if step == 1 else vector_total("xyz"[step - 2])
        if step < 4:
            r["vector_" + "xyz"[step - 1]][0] = total
            start(vector_copies(step))
        else:
            grad_norms[...] = total[:5]
            for k in range(4):
                grad_b2[:, 1024 * k : 1024 * (k + 1)] = total[5 + k : 6 + k]
            grad_b1[...] = total[9:10, :512]
            grad_bo[...] = total[9:10, 512 : 512 + PATCHES]

    start(weights(jnp.int32(0)))
    for name in ("act", "dhid"):
        r[name][ROWS:, :] = jnp.zeros((512 - ROWS, WIDTH), bf16)
    for name in ("dn2", "vector", "columns", "grad_tin", "grad_tout"):
        r[name][...] = jnp.zeros(r[name].shape, f32)
    prologue()
    pl.semaphore_wait(barrier, len(partners))

    def slot_of(t, _):
        @pl.when(t < CHUNKS)
        def _():
            forward(t)

        @pl.when((t >= CHUNKS) & (t < CHUNKS + 2))
        def _():
            token_backward(t - CHUNKS)

        @pl.when(t == CHUNKS + 2)
        def _():
            input_gradients(0)

        tick(t, 0)

        @pl.when(t < CHUNKS)
        def _():
            gradients(t)

        @pl.when((t >= CHUNKS) & (t < CHUNKS + 2))
        def _():
            token_gradients(t - CHUNKS)

        @pl.when(t == CHUNKS + 1)
        def _():
            send_token_gradients()

        @pl.when(t == CHUNKS + 2)
        def _():
            input_gradients(1)
            vector_stage(0)

        tick(t, 1)

        for step in range(1, 5):

            @pl.when(t == CHUNKS + 2 + step)
            def _():
                vector_stage(step)

        return 0

    lax.fori_loop(0, SLOTS, slot_of, 0)
    for b in range(2):
        grad_inputs[b] = r["xs"][b, :PATCHES, :]
    for h in range(2):
        for j in range(CHUNKS):
            for g, out in enumerate((grad_out, grad_in)):
                out[8 * h : 8 * (h + 1), WIDTH * j : WIDTH * (j + 1)] = r["done"][
                    h, j, :, WIDTH * g : WIDTH * (g + 1)
                ]
    grad_tin[...] = r["done_token"][0, :, :PATCHES]
    grad_tout[...] = r["done_token"][1, :, :PATCHES]


def per_device(
    inputs,
    cotangent,
    first_gain,
    first_shift,
    token_in,
    token_in_bias,
    token_out,
    second_gain,
    second_shift,
    channel_in,
    channel_in_bias,
    channel_out,
):
    f32 = jnp.float32
    hidden = channel_in.shape[1]
    shapes = scratch_of()
    names = tuple(shapes)
    vmem, anywhere = pl.BlockSpec(memory_space=pltpu.VMEM), pl.BlockSpec(memory_space=pl.ANY)

    def kernel(*refs):
        block_kernel(names, *refs)

    results = pl.pallas_call(
        kernel,
        out_shape=(
            jax.ShapeDtypeStruct(inputs.shape, jnp.bfloat16),
            jax.ShapeDtypeStruct((8, PATCHES), f32),
            jax.ShapeDtypeStruct((8, PATCHES), f32),
            jax.ShapeDtypeStruct((16, hidden), f32),
            jax.ShapeDtypeStruct((16, hidden), f32),
            jax.ShapeDtypeStruct((5, 1024), f32),
            jax.ShapeDtypeStruct((1, 512), f32),
            jax.ShapeDtypeStruct((1, PATCHES), f32),
            jax.ShapeDtypeStruct((1, hidden), f32),
        ),
        in_specs=[vmem] * 9 + [anywhere, vmem, anywhere],
        out_specs=(vmem,) * 9,
        scratch_shapes=list(shapes.values()),
        compiler_params=pltpu.CompilerParams(collective_id=0, has_side_effects=True, vmem_limit_bytes=67_000_000),
        name="block_backward",
    )(
        inputs,
        cotangent,
        first_gain.reshape(1, -1),
        first_shift.reshape(1, -1),
        token_in,
        token_in_bias.reshape(-1, 1),
        token_out,
        second_gain.reshape(1, -1),
        second_shift.reshape(1, -1),
        channel_in,
        channel_in_bias.reshape(1, -1),
        channel_out,
    )
    return (*results[:6], *(a[0] for a in results[6:]))


def solution(mesh):
    split = Mesh(
        mesh.devices.reshape(mesh.shape["grp"], 4, 2, 4, 2),
        ("grp", "dev_0", "dev_1", "dev_2", "dev_3"),
    )
    in_specs = (
        P(GRP_DEV, None, None),
        P(GRP_DEV, None, None),
        P(),
        P(),
        P(),
        P(),
        P(),
        P(),
        P(),
        P(),
        P(),
        P(),
    )
    out_specs = (
        P(GRP_DEV, None, None),
        P(DEV, None),
        P(DEV, None),
        P(DEV, None),
        P(DEV, None),
        P(),
        P(),
        P(),
        P(),
    )
    return jax.shard_map(
        per_device, mesh=split, in_specs=in_specs, out_specs=out_specs, check_vma=False
    )
```

```python
import math
from typing import Any, NamedTuple

import jax
import jax.numpy as jnp
from jax import lax
from jax.experimental import pallas as pl
from jax.experimental.pallas import tpu as pltpu
from jax.sharding import Mesh
from jax.sharding import PartitionSpec as P

DEV = ("dev_0", "dev_1", "dev_2", "dev_3")
GRP_DEV = ("grp", "dev_0", "dev_1", "dev_2", "dev_3")
MESH = pl.DeviceIdType.MESH

epsilon = 1e-06

AXES = ("x", "y", "z")
CHUNKS = 8
WIDTH = 512
IMAGE = 208
ROWS = 416
PATCHES = 196
COLOURS = (("x", "z", "y", 384), ("y", "z", "x", 384), ("z", "x", "y", 256))
FIRST = (0, 384, 768)
LAG = (0, 0, 2, 4, 6, 8, 10, 12)
LATE = 14
LATE_LAG = (0, 0, 1, 3, 4, 5, 6, 7)
PIECES = CHUNKS + 6
SLOTS = 2 * (CHUNKS - 1) + LAG[-1] + 1
EARLY_SUMS = CHUNKS + 3
LATE_SUMS = CHUNKS + 6


def remainder(a, b):
    return lax.rem(a, jnp.int32(b))


def where_on(fixed, half=None):
    index = [slice(None)] * 4
    for axis, at in fixed.items():
        if axis == "x":
            index[0] = at
        elif axis == "y":
            index[2] = at
        else:
            index[1] = remainder(at, 2)
            index[3] = lax.div(at, jnp.int32(2))
    if half is not None:
        axis, part = half
        if axis == "z_lo":
            index[1] = part
        else:
            index[0 if axis == "x" else 2] = pl.ds(2 * part, 2)
    return tuple(index)


HALVES = (("z_lo", "y"), ("z_lo", "x"), ("x", "y"))
HALF_SHAPES = (((4, 2), (2,)), ((4, 2), (2,)), ((2, 4), (2,)))
BLOCK_SHAPES = (((2, 4, 2), (4,)), ((4, 2, 2), (4,)), ((4, 4), (4,)))


def gelu_parts(v):
    twice = 1.0 + lax.erf(v * (1.0 / math.sqrt(2.0)))
    value = 0.5 * v * twice
    slope = 0.5 * twice + v * jnp.exp(-0.5 * v * v) * (1.0 / math.sqrt(2.0 * math.pi))
    return value, slope


def standardized(values):
    centred = values - jnp.mean(values, axis=-1, keepdims=True)
    rstd = lax.rsqrt(jnp.mean(centred * centred, axis=-1, keepdims=True) + epsilon)
    return centred * rstd, rstd


def norm_backward(incoming, scaled, inv_std, gain):
    weighted = incoming * gain
    first_mean = jnp.mean(weighted, axis=-1, keepdims=True)
    second_mean = jnp.mean(weighted * scaled, axis=-1, keepdims=True)
    return inv_std * (weighted - first_mean - scaled * second_mean)


class Scratch(NamedTuple):
    own: Any
    sums: Any
    half: Any
    block: Any
    last: Any
    done: Any
    done_token: Any
    w_in: Any
    w_out: Any
    act: Any
    dhid: Any
    hid: Any
    dact: Any
    xs: Any
    n1: Any
    act1: Any
    hat2: Any
    rstd2: Any
    n2: Any
    n2t: Any
    cots: Any
    cott: Any
    tin: Any
    tint: Any
    tout: Any
    toutt: Any
    grad_tin: Any
    grad_tout: Any
    dn2: Any
    columns: Any
    bias1: Any
    early: Any
    late: Any
    w_sem: Any
    pair_send: Any
    pair_recv: Any
    half_send: Any
    half_recv: Any
    block_send: Any
    block_recv: Any
    last_send: Any
    last_recv: Any
    both_send: Any
    both_recv: Any
    sums_send: Any
    sums_recv: Any


def scratch_of():
    f32 = lambda *shape: pltpu.VMEM(shape, jnp.float32)
    bf16 = lambda *shape: pltpu.VMEM(shape, jnp.bfloat16)
    dma = lambda *shape: pltpu.SemaphoreType.DMA(shape)
    widths = [colour[3] for colour in COLOURS]
    chunks = [CHUNKS, CHUNKS, CHUNKS + 1]

    def received(shapes):
        return [
            [f32(chunks[c], 2, *shapes[c][p], 8, widths[c]) for p in range(2)] for c in range(3)
        ]

    return Scratch(
        own=[f32(4, 2, 4, 2, 2, 8, w) for w in widths],
        sums=[f32(chunks[c], 4, 2, 4, 2, 8, widths[c]) for c in range(3)],
        half=received(HALF_SHAPES),
        block=received(BLOCK_SHAPES),
        last=[f32(chunks[c], 3, 8, widths[c]) for c in range(3)],
        done=f32(2, CHUNKS, 8, 2 * WIDTH),
        done_token=f32(2, 8, 256),
        w_in=bf16(2, 1024, WIDTH),
        w_out=bf16(2, 1024, WIDTH),
        act=bf16(512, WIDTH),
        dhid=bf16(512, WIDTH),
        hid=f32(512, WIDTH),
        dact=f32(512, WIDTH),
        xs=bf16(2, IMAGE, 1024),
        n1=bf16(2, 256, 1024),
        act1=bf16(2, 512, 1024),
        hat2=f32(ROWS, 1024),
        rstd2=f32(ROWS, 128),
        n2=bf16(512, 1024),
        n2t=bf16(1024, 512),
        cots=bf16(512, 1024),
        cott=bf16(1024, 512),
        tin=bf16(512, 256),
        tint=bf16(256, 512),
        tout=bf16(512, 256),
        toutt=bf16(256, 512),
        grad_tin=f32(512, 256),
        grad_tout=f32(512, 256),
        dn2=f32(ROWS, 1024),
        columns=f32(256, 128),
        bias1=f32(512, 128),
        early=[f32(8, 1024), f32(8, 1024), *(f32(4, 8, 1024) for _ in AXES)],
        late=[f32(8, 384), f32(8, 384), *(f32(4, 8, 384) for _ in AXES)],
        w_sem=dma(2, 2),
        pair_send=dma(CHUNKS + 1, 3),
        pair_recv=dma(CHUNKS + 1, 3),
        half_send=[dma(CHUNKS + 1, 3, 2) for _ in range(2)],
        half_recv=[dma(CHUNKS + 1, 3, 2) for _ in range(2)],
        block_send=[dma(CHUNKS + 1, 3, 2) for _ in range(2)],
        block_recv=[dma(CHUNKS + 1, 3, 2) for _ in range(2)],
        last_send=dma(CHUNKS + 1, 3, 3),
        last_recv=dma(CHUNKS + 1, 3, 3),
        both_send=dma(CHUNKS + 1),
        both_recv=dma(CHUNKS + 1),
        sums_send=dma(2, 4, 3),
        sums_recv=dma(2, 4, 3),
    )


def block_kernel(*refs):
    inputs, cotangent, gain1, shift1, token_in, bias1, token_out, gain2, shift2, win, bias2, wout = refs[:12]
    grad_inputs, grad_tin, grad_tout, grad_in, grad_out, grad_norms, grad_b1, grad_bo, grad_b2 = refs[12:21]
    r = refs[21]
    f32, bf16 = jnp.float32, jnp.bfloat16
    x, y, core = lax.axis_index("dev_0"), lax.axis_index("dev_2"), lax.axis_index("dev_3")
    high = lax.axis_index("grp")
    me = {"x": x, "y": y, "z": 2 * high + lax.axis_index("dev_1")}

    def device(core=core, **moved):
        at = {**me, **moved}
        return (lax.div(at["z"], jnp.int32(2)), at["x"], remainder(at["z"], 2), at["y"], core)

    def along(axis, by):
        return remainder(me[axis] + by, 4)

    partners = [device(core=1 - core)]
    for axis in AXES:
        partners += [device(**{axis: along(axis, by)}) for by in (1, 2, 3)]
    barrier = pltpu.get_barrier_semaphore()
    for partner in partners:
        pl.semaphore_signal(barrier, inc=1, device_id=partner, device_id_type=MESH)

    def remote(source, target, send, recv, to):
        return pltpu.make_async_remote_copy(
            src_ref=source, dst_ref=target, send_sem=send, recv_sem=recv, device_id=to, device_id_type=MESH
        )

    def fixed_before(c, p):
        return {axis: me[axis] for axis in COLOURS[c][:p]}

    def colours(j):
        return (2,) if isinstance(j, int) else (0, 1, 2)

    def pair_copies(j):
        every = slice(None)
        return [
            remote(
                r.own[c].at[every, every, every, 1 - core],
                r.sums[c].at[j],
                r.pair_send.at[j, c],
                r.pair_recv.at[j, c],
                device(core=1 - core),
            )
            for c in colours(j)
        ]

    def half_copies(j, p):
        copies = []
        for c in colours(j):
            axis = COLOURS[c][p]
            for d, by in enumerate((1, 3)):
                spot = where_on({**fixed_before(c, p), axis: along(axis, 2)}, (HALVES[c][p], d))
                copies.append(
                    remote(
                        r.sums[c].at[(j, *spot)],
                        r.half[c][p].at[j, d],
                        r.half_send[p].at[j, c, d],
                        r.half_recv[p].at[j, c, d],
                        device(**{axis: along(axis, by)}),
                    )
                )
        return copies

    def block_copies(j, p):
        copies = []
        for c in colours(j):
            axis = COLOURS[c][p]
            for d, by in enumerate((1, 3)):
                spot = where_on({**fixed_before(c, p), axis: along(axis, by)})
                copies.append(
                    remote(
                        r.sums[c].at[(j, *spot)],
                        r.block[c][p].at[j, d],
                        r.block_send[p].at[j, c, d],
                        r.block_recv[p].at[j, c, d],
                        device(**{axis: along(axis, by)}),
                    )
                )
        return copies

    def last_copies(j):
        copies = []
        for c in colours(j):
            axis = COLOURS[c][2]
            for d, by in enumerate((1, 2, 3)):
                spot = where_on({**fixed_before(c, 2), axis: along(axis, by)})
                copies.append(
                    remote(
                        r.sums[c].at[(j, *spot)],
                        r.last[c].at[j, d],
                        r.last_send.at[j, c, d],
                        r.last_recv.at[j, c, d],
                        device(**{axis: along(axis, by)}),
                    )
                )
        return copies

    def both_copy(j):
        mine = r.done_token.at[high] if isinstance(j, int) else r.done.at[high, j]
        return remote(
            mine,
            mine,
            r.both_send.at[j],
            r.both_recv.at[j],
            device(z=along("z", 2)),
        )

    def start(copies):
        for copy in copies:
            copy.start()

    def wait(copies):
        for copy in copies:
            copy.wait()

    def stage(s, j):
        if s == 1:
            wait(pair_copies(j))
            for c in colours(j):
                for b in range(4):
                    r.sums[c][j, b] += r.own[c][b, :, :, core]
            start(half_copies(j, 0))
        elif s in (2, 4):
            p = s // 2 - 1
            wait(half_copies(j, p))
            for c in colours(j):
                axis = COLOURS[c][p]
                for d, by in enumerate((1, 3)):
                    spot = where_on({**fixed_before(c, p), axis: along(axis, by)}, (HALVES[c][p], d))
                    r.sums[c][(j, *spot)] += r.half[c][p][j, d]
            start(block_copies(j, p))
        elif s in (3, 5):
            p = s // 2 - 1
            wait(block_copies(j, p))
            for c in colours(j):
                spot = where_on(fixed_before(c, p + 1))
                r.sums[c][(j, *spot)] += r.block[c][p][j, 0] + r.block[c][p][j, 1]
            start(half_copies(j, 1) if p == 0 else last_copies(j))
        elif s == 6:
            wait(last_copies(j))
            for c in colours(j):
                width = COLOURS[c][3]
                spot = where_on(me)
                got = r.last[c]
                total = r.sums[c][(j, *spot)] + got[j, 0] + (got[j, 1] + got[j, 2])
                if isinstance(j, int):
                    r.done_token[high] = total
                else:
                    r.done[high, j, :, FIRST[c] : FIRST[c] + width] = total
            start([both_copy(j)])
        else:
            wait([both_copy(j)])

    def serve(t):
        for s in range(7, 1, -1):
            from_start = t - LAG[s]
            j = lax.div(from_start, jnp.int32(2))

            @pl.when((from_start >= 0) & (from_start < 2 * CHUNKS) & (remainder(from_start + 2 * CHUNKS, 2) == 0))
            def _():
                stage(s, j)

            @pl.when(t == LATE + LATE_LAG[s])
            def _():
                stage(s, CHUNKS)

    def weights(j):
        slot = remainder(j, 2)
        columns = pl.ds(pl.multiple_of(j * WIDTH, WIDTH), WIDTH)
        return [
            pltpu.make_async_copy(win.at[:, columns], r.w_in.at[slot], r.w_sem.at[slot, 0]),
            pltpu.make_async_copy(wout.at[:, columns], r.w_out.at[slot], r.w_sem.at[slot, 1]),
        ]

    act, dhid, hid, dact, dn2 = r.act, r.dhid, r.hid, r.dact, r.dn2
    early, late = r.early[0], r.late[0]

    def blocks_of(count, size, step, carry=0, group=1):
        def at_block(i, carry):
            for u in range(group):
                n = i * group + u
                carry = step(pl.ds(pl.multiple_of(n * size, size), size), n, carry)
            return carry

        carry = lax.fori_loop(0, count // group, at_block, carry)
        for n in range(count // group * group, count):
            carry = step(pl.ds(n * size, size), n, carry)
        return carry

    def real(i):
        return lax.broadcasted_iota(jnp.int32, (16, 1), 0) + 16 * i < PATCHES

    def folded(values):
        return jnp.sum(values.reshape(2, 8, 1024), axis=0)

    def rows_of(b, i):
        return pl.ds(pl.multiple_of(IMAGE * b + 16 * i, 16), 16)

    def columns_of(half):
        return slice(512 * half, 512 * (half + 1))

    def dh1(b, half):
        return r.w_in.at[b, columns_of(half), :]

    def dmr(b, half):
        return r.w_out.at[b, 256 * half : 256 * (half + 1), :]

    def token_hidden(b, columns):
        hid[...] = jnp.dot(r.tin[...], r.n1[b, :, columns], preferred_element_type=f32)

    def both_images(ref, i, whole=True):
        if whole:
            values = ref[pl.ds(pl.multiple_of(16 * i, 16), 16)].astype(f32)
            return [values[:, b, :] for b in range(2)]
        values = ref[192:PATCHES].astype(f32)
        blocks = []
        for b in range(2):
            spot = r.hat2.at[16 * b : 16 * (b + 1), :]
            spot[...] = jnp.zeros((16, 1024), f32)
            spot[: PATCHES - 192, :] = values[:, b, :]
            blocks.append(spot[...])
        return blocks

    def prologue():
        for direct, turned, ref in ((r.tin, r.tint, token_in), (r.tout, r.toutt, token_out)):
            turned[192:, :] = jnp.zeros((64, 512), bf16)
            turned[:PATCHES, :] = ref[...]
            direct[...] = turned[...].T
        r.bias1[...] = jnp.broadcast_to(bias1[...], (128, 512)).T
        for b in range(2):
            r.n1[b, IMAGE:, :] = jnp.zeros((256 - IMAGE, 1024), bf16)
        gain, shift = gain1[...], shift1[...]

        def first_norm(at, i, _, whole=True):
            for b, values in enumerate(both_images(inputs, i, whole)):
                r.xs[b, at, :] = values.astype(bf16)
                value = standardized(values)[0] * gain + shift
                r.n1[b, at, :] = (value if whole else jnp.where(real(i), value, 0.0)).astype(bf16)
            return 0

        blocks_of(12, 16, first_norm, group=3)
        first_norm(pl.ds(192, 16), 12, 0, False)

        def split(at, i, _, whole=True):
            for b, values in enumerate(both_images(cotangent, i, whole)):
                r.cots[rows_of(b, i), :] = values.astype(bf16)
            return 0

        blocks_of(12, 16, split, group=3)
        split(None, 12, 0, False)
        r.cots[ROWS:, :] = jnp.zeros((512 - ROWS, 1024), bf16)
        r.n2[ROWS:, :] = jnp.zeros((512 - ROWS, 1024), bf16)
        for b in range(2):
            for half in range(2):
                columns = columns_of(half)
                token_hidden(b, columns)

                def activate(at, i, _):
                    value = gelu_parts(hid[at, :] + r.bias1[at, :1])[0]
                    r.act1[b, at, columns] = value.astype(bf16)
                    return 0

                blocks_of(16, 32, activate, group=2)
            for half in range(2):
                columns = columns_of(half)
                r.hat2[IMAGE * b : IMAGE * (b + 1), columns] = jnp.dot(
                    r.toutt[:IMAGE, :], r.act1[b, :, columns], preferred_element_type=f32
                )
        r.cott[...] = r.cots[...].T
        gain, shift = gain2[...], shift2[...]

        def second_norm(at, i, _):
            for b in range(2):
                rows = rows_of(b, i)
                hat, rstd = standardized(r.xs[b, at, :].astype(f32) + r.hat2[rows, :])
                r.hat2[rows, :] = hat
                r.rstd2[rows, :] = jnp.broadcast_to(rstd, (16, 128))
                r.n2[rows, :] = jnp.where(real(i), hat * gain + shift, 0.0).astype(bf16)
            return 0

        blocks_of(13, 16, second_norm, group=3)
        r.n2t[...] = r.n2[...].T

    def forward(j):
        slot = remainder(j, 2)
        wait(weights(j))

        @pl.when(j + 1 < CHUNKS)
        def _():
            start(weights(j + 1))

        columns = pl.ds(pl.multiple_of(j * WIDTH, WIDTH), WIDTH)
        for b in range(WIDTH // 256):
            part = slice(256 * b, 256 * (b + 1))
            hid[:ROWS, part] = jnp.dot(r.n2[:ROWS, :], r.w_in[slot, :, part], preferred_element_type=f32)
            dact[:ROWS, part] = jnp.dot(r.cots[:ROWS, :], r.w_out[slot, :, part], preferred_element_type=f32)
        shift = bias2[:, columns]

        def rows(at, i, total):
            value, slope = gelu_parts(hid[at, :] + shift)
            act[at, :] = value.astype(bf16)
            d = (dact[at, :] * slope).astype(bf16)
            dhid[at, :] = d
            return total + jnp.sum(d.astype(f32).reshape(4, 8, WIDTH), axis=0)

        total = blocks_of(ROWS // 32, 32, rows, jnp.zeros((8, WIDTH), f32))
        early[pl.ds(j, 1), :WIDTH] = jnp.sum(total, axis=0, keepdims=True)

    def gradients(j):
        slot = remainder(j, 2)

        def rows(at, i, _):
            out = jnp.dot(r.cott[at, :], act[...], preferred_element_type=f32).reshape(2, 4, 2, 2, 8, WIDTH)
            r.own[0][i] = out[..., :384]
            r.own[1][i, :, :, :, :, :, :128] = out[..., 384:]
            inn = jnp.dot(r.n2t[at, :], dhid[...], preferred_element_type=f32).reshape(2, 4, 2, 2, 8, WIDTH)
            r.own[1][i, :, :, :, :, :, 128:] = inn[..., :256]
            r.own[2][i] = inn[..., 256:]
            return 0

        blocks_of(4, 256, rows)
        start(pair_copies(j))
        for b in range(4):
            part = slice(256 * b, 256 * (b + 1))
            dn2[:, part] += lax.dot_general(
                dhid[:ROWS, :],
                r.w_in[slot, part, :],
                (((1,), (1,)), ((), ())),
                preferred_element_type=f32,
            )

    def across(a, b):
        return lax.dot_general(a, b, (((1,), (1,)), ((), ())), preferred_element_type=f32)

    def fold_into(ref, row, lane, total):
        summed = jnp.sum(total, axis=0, keepdims=True)
        for k in range(4):
            ref[row + k : row + k + 1, lane : lane + 256] += summed[:, 256 * k : 256 * (k + 1)]

    def token_backward(b):
        gain = gain2[...]
        for half in range(2):
            dmr(b, half)[IMAGE:, :] = jnp.zeros((256 - IMAGE, 512), bf16)

        def second_norm(at, i, sums):
            rows = rows_of(b, i)
            hat, incoming = r.hat2[rows, :], dn2[rows, :]
            g = r.cots[rows, :].astype(f32)
            dmixed = g + norm_backward(incoming, hat, r.rstd2[rows, :1], gain)
            dn2[rows, :] = dmixed
            rounded = dmixed.astype(bf16)
            for half in range(2):
                dmr(b, half)[at, :] = rounded[:, columns_of(half)]
            r.columns[at, :] += jnp.broadcast_to(jnp.sum(dmixed, axis=1, keepdims=True), (16, 128))
            return (sums[0] + folded(incoming * hat), sums[1] + folded(incoming), sums[2] + folded(g))

        zero = jnp.zeros((8, 1024), f32)
        sums = blocks_of(13, 16, second_norm, (zero, zero, zero), group=2)
        fold_into(early, 0, 512, sums[0])
        fold_into(early, 4, 512, sums[1])
        fold_into(early, 0, 768, sums[2])
        for half in range(2):
            token_hidden(b, columns_of(half))
            dact[...] = jnp.dot(r.tout[...], dmr(b, half)[...], preferred_element_type=f32)

            def back(at, i, _):
                slope = gelu_parts(hid[at, :] + r.bias1[at, :1])[1]
                dh1(b, half)[at, :] = (dact[at, :] * slope).astype(bf16)
                return 0

            blocks_of(16, 32, back)

    def token_gradients(b):
        ones = jnp.ones((8, 512), bf16)
        for half in range(2):
            columns = columns_of(half)
            r.grad_tin[...] += across(dh1(b, half)[...], r.n1[b, :, columns])
            r.grad_tout[...] += across(r.act1[b, :, columns], dmr(b, half)[...])
            total = across(ones, dh1(b, half)[...])[:1]
            for k in range(4):
                late[k : k + 1, 256:] += total[:, 128 * k : 128 * (k + 1)]

    def send_token_gradients():
        for h, grad in enumerate((r.grad_tin, r.grad_tout)):
            r.own[2][:, :, :, :, h] = grad[...].reshape(4, 2, 4, 2, 8, 256)
        start(pair_copies(CHUNKS))

    def input_gradients(b):
        gain = gain1[...]
        for half in range(2):
            r.hat2[:IMAGE, columns_of(half)] = jnp.dot(
                r.tint[:IMAGE, :], dh1(b, half)[...], preferred_element_type=f32
            )

        def first_norm(at, i, sums):
            hat, rstd = standardized(r.xs[b, at, :].astype(f32))
            incoming = r.hat2[at, :]
            rows = rows_of(b, i)
            dn2[rows, :] += norm_backward(incoming, hat, rstd, gain)
            return (sums[0] + folded(incoming * hat), sums[1] + folded(incoming))

        zero = jnp.zeros((8, 1024), f32)
        sums = blocks_of(13, 16, first_norm, (zero, zero), group=2)
        fold_into(late, 0, 0, sums[0])
        fold_into(late, 4, 0, sums[1])

    def interleave():
        def rows(at, i, _):
            both = [dn2[pl.ds(pl.multiple_of(IMAGE * b + 8 * i, 8), 8), :] for b in range(2)]
            grad_inputs[pl.ds(pl.multiple_of(8 * i, 8), 8)] = jnp.stack(both, axis=1).astype(bf16)
            return 0

        blocks_of(24, 8, rows)
        both = [dn2[IMAGE * b + 192 : IMAGE * b + 200, :][: PATCHES - 192] for b in range(2)]
        grad_inputs[192:PATCHES] = jnp.stack(both, axis=1).astype(bf16)

    def sums_copies(which, step):
        at = (r.early, r.late)[which]
        send, recv = r.sums_send.at[which, step], r.sums_recv.at[which, step]
        if step == 0:
            return [remote(at[0], at[1], send.at[0], recv.at[0], device(core=1 - core))]
        axis, ring = AXES[step - 1], at[step + 1]
        return [
            remote(ring.at[0], ring.at[by], send.at[by - 1], recv.at[by - 1], device(**{axis: along(axis, by)}))
            for by in (1, 2, 3)
        ]

    def sums_stage(which, step):
        at = (r.early, r.late)[which]
        if step == 0:
            start(sums_copies(which, 0))
            return None
        wait(sums_copies(which, step - 1))
        if step == 1:
            total = at[0][...] + at[1][...]
        else:
            ring, mine = at[step], me[AXES[step - 2]]
            terms = [ring[remainder(mine + 4 - k, 4)] for k in range(4)]
            total = (terms[0] + terms[1]) + (terms[2] + terms[3])
        if step < 4:
            at[step + 1][0] = total
            start(sums_copies(which, step))
        return total

    def unfold(total, row, lane):
        return [total[row + k : row + k + 1, lane : lane + 256] for k in range(4)]

    def finish_early(total):
        for j in range(CHUNKS):
            grad_b2[:, WIDTH * j : WIDTH * (j + 1)] = total[j : j + 1, :WIDTH]
        for n, (row, lane) in ((2, (0, 512)), (3, (4, 512)), (4, (0, 768))):
            for k, part in enumerate(unfold(total, row, lane)):
                grad_norms[n : n + 1, 256 * k : 256 * (k + 1)] = part
        grad_bo[...] = total[4:5, 768 : 768 + PATCHES]

    def finish_late(total):
        for n, row in ((0, 0), (1, 4)):
            for k, part in enumerate(unfold(total, row, 0)):
                grad_norms[n : n + 1, 256 * k : 256 * (k + 1)] = part
        for k in range(4):
            grad_b1[:, 128 * k : 128 * (k + 1)] = total[k : k + 1, 256:]

    start(weights(jnp.int32(0)))
    for ref in (act, dhid):
        ref[ROWS:, :] = jnp.zeros((512 - ROWS, WIDTH), bf16)
    for ref in (dn2, early, late, r.columns, r.grad_tin, r.grad_tout):
        ref[...] = jnp.zeros(ref.shape, f32)
    prologue()
    pl.semaphore_wait(barrier, len(partners))

    def slot_of(t, _):
        @pl.when(t < CHUNKS)
        def _():
            forward(t)

        @pl.when((t >= 1) & (t <= CHUNKS))
        def _():
            stage(1, t - 1)

        @pl.when(t < CHUNKS)
        def _():
            gradients(t)

        @pl.when((t >= CHUNKS) & (t < CHUNKS + 2))
        def _():
            token_backward(t - CHUNKS)

        @pl.when((t >= CHUNKS + 2) & (t < CHUNKS + 4))
        def _():
            token_gradients(t - CHUNKS - 2)

        @pl.when(t == CHUNKS + 3)
        def _():
            send_token_gradients()

        @pl.when(t == CHUNKS + 4)
        def _():
            stage(1, CHUNKS)

        @pl.when((t >= CHUNKS + 4) & (t < CHUNKS + 6))
        def _():
            input_gradients(t - CHUNKS - 4)

        @pl.when(t == EARLY_SUMS)
        def _():
            early[4:5, 768:] = r.columns[...].T[:1, :]

        for step in range(4):
            for which, first in enumerate((EARLY_SUMS, LATE_SUMS)):

                @pl.when(t == first + step)
                def _():
                    sums_stage(which, step)

        serve(t)

        @pl.when(t == LATE_SUMS + 1)
        def _():
            interleave()

        return 0

    lax.fori_loop(0, SLOTS, slot_of, 0)
    finish_early(sums_stage(0, 4))
    finish_late(sums_stage(1, 4))
    for h in range(2):
        for j in range(CHUNKS):
            for g, out in enumerate((grad_out, grad_in)):
                out[8 * h : 8 * (h + 1), WIDTH * j : WIDTH * (j + 1)] = r.done[
                    h, j, :, WIDTH * g : WIDTH * (g + 1)
                ]
    grad_tin[...] = r.done_token[0, :, :PATCHES]
    grad_tout[...] = r.done_token[1, :, :PATCHES]


def hand_over(*refs):
    count = len(refs) // 2
    for source, target in zip(refs[:count], refs[count:]):
        target[...] = source[...]


def per_device(
    inputs,
    cotangent,
    first_gain,
    first_shift,
    token_in,
    token_in_bias,
    token_out,
    second_gain,
    second_shift,
    channel_in,
    channel_in_bias,
    channel_out,
):
    f32 = jnp.float32
    hidden = channel_in.shape[1]
    vmem, anywhere = pl.BlockSpec(memory_space=pltpu.VMEM), pl.BlockSpec(memory_space=pl.ANY)

    results = pl.pallas_call(
        block_kernel,
        out_shape=(
            jax.ShapeDtypeStruct((PATCHES, 2, 1024), jnp.bfloat16),
            jax.ShapeDtypeStruct((8, PATCHES), f32),
            jax.ShapeDtypeStruct((8, PATCHES), f32),
            jax.ShapeDtypeStruct((16, hidden), f32),
            jax.ShapeDtypeStruct((16, hidden), f32),
            jax.ShapeDtypeStruct((5, 1024), f32),
            jax.ShapeDtypeStruct((1, 512), f32),
            jax.ShapeDtypeStruct((1, PATCHES), f32),
            jax.ShapeDtypeStruct((1, hidden), f32),
        ),
        in_specs=[vmem] * 9 + [anywhere, vmem, anywhere],
        out_specs=(vmem,) * 9,
        scratch_shapes=(scratch_of(),),
        compiler_params=pltpu.CompilerParams(collective_id=0, has_side_effects=True, vmem_limit_bytes=67_000_000),
        name="block_backward",
    )(
        inputs.swapaxes(0, 1),
        cotangent.swapaxes(0, 1),
        first_gain.reshape(1, -1),
        first_shift.reshape(1, -1),
        token_in.T,
        token_in_bias.reshape(1, -1),
        token_out.T,
        second_gain.reshape(1, -1),
        second_shift.reshape(1, -1),
        channel_in,
        channel_in_bias.reshape(1, -1),
        channel_out,
    )
    results = pl.pallas_call(
        hand_over,
        out_shape=tuple(jax.ShapeDtypeStruct(a.shape, a.dtype) for a in results),
        in_specs=[vmem] * 9,
        out_specs=(vmem,) * 9,
        name="hand_over",
    )(*results)
    return (results[0].swapaxes(0, 1), *results[1:6], *(a[0] for a in results[6:]))


def solution(mesh):
    split = Mesh(
        mesh.devices.reshape(mesh.shape["grp"], 4, 2, 4, 2),
        ("grp", "dev_0", "dev_1", "dev_2", "dev_3"),
    )
    in_specs = (
        P(GRP_DEV, None, None),
        P(GRP_DEV, None, None),
        P(),
        P(),
        P(),
        P(),
        P(),
        P(),
        P(),
        P(),
        P(),
        P(),
    )
    out_specs = (
        P(GRP_DEV, None, None),
        P(DEV, None),
        P(DEV, None),
        P(DEV, None),
        P(DEV, None),
        P(),
        P(),
        P(),
        P(),
    )
    return jax.shard_map(
        per_device, mesh=split, in_specs=in_specs, out_specs=out_specs, check_vma=False
    )
```

```python
import math
from typing import Any, NamedTuple

import jax
import jax.numpy as jnp
from jax import lax
from jax.experimental import pallas as pl
from jax.experimental.pallas import tpu as pltpu
from jax.sharding import Mesh
from jax.sharding import PartitionSpec as P

DEV = ("dev_0", "dev_1", "dev_2", "dev_3")
GRP_DEV = ("grp", "dev_0", "dev_1", "dev_2", "dev_3")
MESH = pl.DeviceIdType.MESH

epsilon = 1e-06

AXES = ("x", "y", "z")
CHUNKS = 8
WIDTH = 512
IMAGE = 208
ROWS = 416
PATCHES = 196
COLOURS = (("x", "z", "y", 384), ("y", "z", "x", 384), ("z", "x", "y", 256))
FIRST = (0, 384, 768)
LAG = (0, 2, 5, 8, 11, 14, 17, 20)
AFTER = 2 * CHUNKS
LATE_SLOT = (0, 20, 22, 25, 27, 29, 32, 34)
SLOTS = 2 * (CHUNKS - 1) + LAG[-1] + 1
EARLY_SUMS = AFTER + 2
LATE_SUMS = AFTER + 6


def remainder(a, b):
    return lax.rem(a, jnp.int32(b))


def where_on(fixed, half=None):
    index = [slice(None)] * 4
    for axis, at in fixed.items():
        if axis == "x":
            index[0] = at
        elif axis == "y":
            index[2] = at
        else:
            index[1] = remainder(at, 2)
            index[3] = lax.div(at, jnp.int32(2))
    if half is not None:
        axis, part = half
        if axis == "z_lo":
            index[1] = part
        else:
            index[0 if axis == "x" else 2] = pl.ds(2 * part, 2)
    return tuple(index)


HALVES = (("z_lo", "y"), ("z_lo", "x"), ("x", "y"))
HALF_SHAPES = (((4, 2), (2,)), ((4, 2), (2,)), ((2, 4), (2,)))
BLOCK_SHAPES = (((2, 4, 2), (4,)), ((4, 2, 2), (4,)), ((4, 4), (4,)))


def gelu_parts(v):
    twice = 1.0 + lax.erf(v * (1.0 / math.sqrt(2.0)))
    value = 0.5 * v * twice
    slope = 0.5 * twice + v * jnp.exp(-0.5 * v * v) * (1.0 / math.sqrt(2.0 * math.pi))
    return value, slope


def standardized(values):
    centred = values - jnp.mean(values, axis=-1, keepdims=True)
    rstd = lax.rsqrt(jnp.mean(centred * centred, axis=-1, keepdims=True) + epsilon)
    return centred * rstd, rstd


def norm_backward(incoming, scaled, inv_std, gain):
    weighted = incoming * gain
    first_mean = jnp.mean(weighted, axis=-1, keepdims=True)
    second_mean = jnp.mean(weighted * scaled, axis=-1, keepdims=True)
    return inv_std * (weighted - first_mean - scaled * second_mean)


class Scratch(NamedTuple):
    own: Any
    sums: Any
    half: Any
    block: Any
    last: Any
    done: Any
    done_token: Any
    w_in: Any
    w_out: Any
    act: Any
    dhid: Any
    hid: Any
    dact: Any
    xs: Any
    n1: Any
    act1: Any
    hat2: Any
    rstd2: Any
    n2: Any
    n2t: Any
    cots: Any
    cott: Any
    tin: Any
    tint: Any
    tout: Any
    toutt: Any
    grad_tin: Any
    grad_tout: Any
    dn2: Any
    columns: Any
    bias1: Any
    early: Any
    late: Any
    w_sem: Any
    pair_send: Any
    pair_recv: Any
    half_send: Any
    half_recv: Any
    block_send: Any
    block_recv: Any
    last_send: Any
    last_recv: Any
    both_send: Any
    both_recv: Any
    sums_send: Any
    sums_recv: Any


def scratch_of():
    f32 = lambda *shape: pltpu.VMEM(shape, jnp.float32)
    bf16 = lambda *shape: pltpu.VMEM(shape, jnp.bfloat16)
    dma = lambda *shape: pltpu.SemaphoreType.DMA(shape)
    widths = [colour[3] for colour in COLOURS]
    chunks = [CHUNKS, CHUNKS, CHUNKS + 1]

    def received(shapes):
        return [
            [f32(chunks[c], 2, *shapes[c][p], 8, widths[c]) for p in range(2)] for c in range(3)
        ]

    return Scratch(
        own=[f32(4, 2, 4, 2, 2, 8, w) for w in widths],
        sums=[f32(chunks[c], 4, 2, 4, 2, 8, widths[c]) for c in range(3)],
        half=received(HALF_SHAPES),
        block=received(BLOCK_SHAPES),
        last=[f32(chunks[c], 3, 8, widths[c]) for c in range(3)],
        done=f32(2, CHUNKS, 8, 2 * WIDTH),
        done_token=f32(2, 8, 256),
        w_in=bf16(2, 1024, WIDTH),
        w_out=bf16(2, 1024, WIDTH),
        act=bf16(512, WIDTH),
        dhid=bf16(512, WIDTH),
        hid=f32(512, WIDTH),
        dact=f32(512, WIDTH),
        xs=bf16(2, IMAGE, 1024),
        n1=bf16(2, 256, 1024),
        act1=bf16(2, 512, 1024),
        hat2=f32(ROWS, 1024),
        rstd2=f32(ROWS, 128),
        n2=bf16(512, 1024),
        n2t=bf16(1024, 512),
        cots=bf16(512, 1024),
        cott=bf16(1024, 512),
        tin=bf16(512, 256),
        tint=bf16(256, 512),
        tout=bf16(512, 256),
        toutt=bf16(256, 512),
        grad_tin=f32(512, 256),
        grad_tout=f32(512, 256),
        dn2=f32(ROWS, 1024),
        columns=f32(256, 128),
        bias1=f32(512, 128),
        early=[f32(8, 1024), f32(8, 1024), *(f32(4, 8, 1024) for _ in AXES)],
        late=[f32(8, 384), f32(8, 384), *(f32(4, 8, 384) for _ in AXES)],
        w_sem=dma(2, 2),
        pair_send=dma(CHUNKS + 1, 3),
        pair_recv=dma(CHUNKS + 1, 3),
        half_send=[dma(CHUNKS + 1, 3, 2) for _ in range(2)],
        half_recv=[dma(CHUNKS + 1, 3, 2) for _ in range(2)],
        block_send=[dma(CHUNKS + 1, 3, 2) for _ in range(2)],
        block_recv=[dma(CHUNKS + 1, 3, 2) for _ in range(2)],
        last_send=dma(CHUNKS + 1, 3, 3),
        last_recv=dma(CHUNKS + 1, 3, 3),
        both_send=dma(CHUNKS + 1),
        both_recv=dma(CHUNKS + 1),
        sums_send=dma(2, 4, 3),
        sums_recv=dma(2, 4, 3),
    )


def block_kernel(*refs):
    inputs, cotangent, gain1, shift1, token_in, bias1, token_out, gain2, shift2, win, bias2, wout = refs[:12]
    grad_inputs, grad_tin, grad_tout, grad_in, grad_out, grad_norms, grad_b1, grad_bo, grad_b2 = refs[12:21]
    r = refs[21]
    f32, bf16 = jnp.float32, jnp.bfloat16
    x, y, core = lax.axis_index("dev_0"), lax.axis_index("dev_2"), lax.axis_index("dev_3")
    high = lax.axis_index("grp")
    me = {"x": x, "y": y, "z": 2 * high + lax.axis_index("dev_1")}

    def device(core=core, **moved):
        at = {**me, **moved}
        return (lax.div(at["z"], jnp.int32(2)), at["x"], remainder(at["z"], 2), at["y"], core)

    def along(axis, by):
        return remainder(me[axis] + by, 4)

    partners = [device(core=1 - core)]
    for axis in AXES:
        partners += [device(**{axis: along(axis, by)}) for by in (1, 2, 3)]
    barrier = pltpu.get_barrier_semaphore()
    for partner in partners:
        pl.semaphore_signal(barrier, inc=1, device_id=partner, device_id_type=MESH)

    def remote(source, target, send, recv, to):
        return pltpu.make_async_remote_copy(
            src_ref=source, dst_ref=target, send_sem=send, recv_sem=recv, device_id=to, device_id_type=MESH
        )

    def fixed_before(c, p):
        return {axis: me[axis] for axis in COLOURS[c][:p]}

    def colours(j):
        return (2,) if isinstance(j, int) else (0, 1, 2)

    def pair_copies(j):
        every = slice(None)
        return [
            remote(
                r.own[c].at[every, every, every, 1 - core],
                r.sums[c].at[j],
                r.pair_send.at[j, c],
                r.pair_recv.at[j, c],
                device(core=1 - core),
            )
            for c in colours(j)
        ]

    def half_copies(j, p):
        copies = []
        for c in colours(j):
            axis = COLOURS[c][p]
            for d, by in enumerate((1, 3)):
                spot = where_on({**fixed_before(c, p), axis: along(axis, 2)}, (HALVES[c][p], d))
                copies.append(
                    remote(
                        r.sums[c].at[(j, *spot)],
                        r.half[c][p].at[j, d],
                        r.half_send[p].at[j, c, d],
                        r.half_recv[p].at[j, c, d],
                        device(**{axis: along(axis, by)}),
                    )
                )
        return copies

    def block_copies(j, p):
        copies = []
        for c in colours(j):
            axis = COLOURS[c][p]
            for d, by in enumerate((1, 3)):
                spot = where_on({**fixed_before(c, p), axis: along(axis, by)})
                copies.append(
                    remote(
                        r.sums[c].at[(j, *spot)],
                        r.block[c][p].at[j, d],
                        r.block_send[p].at[j, c, d],
                        r.block_recv[p].at[j, c, d],
                        device(**{axis: along(axis, by)}),
                    )
                )
        return copies

    def last_copies(j):
        copies = []
        for c in colours(j):
            axis = COLOURS[c][2]
            for d, by in enumerate((1, 2, 3)):
                spot = where_on({**fixed_before(c, 2), axis: along(axis, by)})
                copies.append(
                    remote(
                        r.sums[c].at[(j, *spot)],
                        r.last[c].at[j, d],
                        r.last_send.at[j, c, d],
                        r.last_recv.at[j, c, d],
                        device(**{axis: along(axis, by)}),
                    )
                )
        return copies

    def both_copy(j):
        mine = r.done_token.at[high] if isinstance(j, int) else r.done.at[high, j]
        return remote(
            mine,
            mine,
            r.both_send.at[j],
            r.both_recv.at[j],
            device(z=along("z", 2)),
        )

    def start(copies):
        for copy in copies:
            copy.start()

    def wait(copies):
        for copy in copies:
            copy.wait()

    def stage(s, j):
        if s == 1:
            wait(pair_copies(j))
            for c in colours(j):
                for b in range(4):
                    r.sums[c][j, b] += r.own[c][b, :, :, core]
            start(half_copies(j, 0))
        elif s in (2, 4):
            p = s // 2 - 1
            wait(half_copies(j, p))
            for c in colours(j):
                axis = COLOURS[c][p]
                for d, by in enumerate((1, 3)):
                    spot = where_on({**fixed_before(c, p), axis: along(axis, by)}, (HALVES[c][p], d))
                    r.sums[c][(j, *spot)] += r.half[c][p][j, d]
            start(block_copies(j, p))
        elif s in (3, 5):
            p = s // 2 - 1
            wait(block_copies(j, p))
            for c in colours(j):
                spot = where_on(fixed_before(c, p + 1))
                r.sums[c][(j, *spot)] += r.block[c][p][j, 0] + r.block[c][p][j, 1]
            start(half_copies(j, 1) if p == 0 else last_copies(j))
        elif s == 6:
            wait(last_copies(j))
            for c in colours(j):
                width = COLOURS[c][3]
                spot = where_on(me)
                got = r.last[c]
                total = r.sums[c][(j, *spot)] + got[j, 0] + (got[j, 1] + got[j, 2])
                if isinstance(j, int):
                    r.done_token[high] = total
                else:
                    r.done[high, j, :, FIRST[c] : FIRST[c] + width] = total
            start([both_copy(j)])
        else:
            wait([both_copy(j)])

    def serve(t):
        for s in range(7, 0, -1):
            from_start = t - LAG[s]
            j = lax.div(from_start, jnp.int32(2))

            @pl.when((from_start >= 0) & (from_start < 2 * CHUNKS) & (remainder(from_start + 4 * CHUNKS, 2) == 0))
            def _():
                stage(s, j)

            @pl.when(t == LATE_SLOT[s])
            def _():
                stage(s, CHUNKS)

    def weights(j):
        slot = remainder(j, 2)
        columns = pl.ds(pl.multiple_of(j * WIDTH, WIDTH), WIDTH)
        return [
            pltpu.make_async_copy(win.at[:, columns], r.w_in.at[slot], r.w_sem.at[slot, 0]),
            pltpu.make_async_copy(wout.at[:, columns], r.w_out.at[slot], r.w_sem.at[slot, 1]),
        ]

    act, dhid, hid, dact, dn2 = r.act, r.dhid, r.hid, r.dact, r.dn2
    early, late = r.early[0], r.late[0]

    def blocks_of(count, size, step, carry=0, group=1):
        def at_block(i, carry):
            for u in range(group):
                n = i * group + u
                carry = step(pl.ds(pl.multiple_of(n * size, size), size), n, carry)
            return carry

        carry = lax.fori_loop(0, count // group, at_block, carry)
        for n in range(count // group * group, count):
            carry = step(pl.ds(n * size, size), n, carry)
        return carry

    def real(i):
        return lax.broadcasted_iota(jnp.int32, (16, 1), 0) + 16 * i < PATCHES

    def folded(values):
        return jnp.sum(values.reshape(2, 8, 1024), axis=0)

    def rows_of(b, i):
        return pl.ds(pl.multiple_of(IMAGE * b + 16 * i, 16), 16)

    def columns_of(half):
        return slice(512 * half, 512 * (half + 1))

    def dh1(b, half):
        return r.w_in.at[b, columns_of(half), :]

    def dmr(b, half):
        return r.w_out.at[b, 256 * half : 256 * (half + 1), :]

    def token_hidden(b, columns):
        hid[...] = jnp.dot(r.tin[...], r.n1[b, :, columns], preferred_element_type=f32)

    def both_images(ref, i, whole=True):
        if whole:
            values = ref[pl.ds(pl.multiple_of(16 * i, 16), 16)].astype(f32)
            return [values[:, b, :] for b in range(2)]
        values = ref[192:PATCHES].astype(f32)
        blocks = []
        for b in range(2):
            spot = r.hat2.at[16 * b : 16 * (b + 1), :]
            spot[...] = jnp.zeros((16, 1024), f32)
            spot[: PATCHES - 192, :] = values[:, b, :]
            blocks.append(spot[...])
        return blocks

    def prologue():
        for direct, turned, ref in ((r.tin, r.tint, token_in), (r.tout, r.toutt, token_out)):
            turned[192:, :] = jnp.zeros((64, 512), bf16)
            turned[:PATCHES, :] = ref[...]
            direct[...] = turned[...].T
        r.bias1[...] = jnp.broadcast_to(bias1[...], (128, 512)).T
        for b in range(2):
            r.n1[b, IMAGE:, :] = jnp.zeros((256 - IMAGE, 1024), bf16)
        gain, shift = gain1[...], shift1[...]

        def first_norm(at, i, _, whole=True):
            for b, values in enumerate(both_images(inputs, i, whole)):
                r.xs[b, at, :] = values.astype(bf16)
                value = standardized(values)[0] * gain + shift
                r.n1[b, at, :] = (value if whole else jnp.where(real(i), value, 0.0)).astype(bf16)
            return 0

        blocks_of(12, 16, first_norm, group=3)
        first_norm(pl.ds(192, 16), 12, 0, False)

        def split(at, i, _, whole=True):
            for b, values in enumerate(both_images(cotangent, i, whole)):
                r.cots[rows_of(b, i), :] = values.astype(bf16)
            return 0

        blocks_of(12, 16, split, group=3)
        split(None, 12, 0, False)
        r.cots[ROWS:, :] = jnp.zeros((512 - ROWS, 1024), bf16)
        r.n2[ROWS:, :] = jnp.zeros((512 - ROWS, 1024), bf16)
        for b in range(2):
            for half in range(2):
                columns = columns_of(half)
                token_hidden(b, columns)

                def activate(at, i, _):
                    value = gelu_parts(hid[at, :] + r.bias1[at, :1])[0]
                    r.act1[b, at, columns] = value.astype(bf16)
                    return 0

                blocks_of(16, 32, activate, group=2)
            for half in range(2):
                columns = columns_of(half)
                r.hat2[IMAGE * b : IMAGE * (b + 1), columns] = jnp.dot(
                    r.toutt[:IMAGE, :], r.act1[b, :, columns], preferred_element_type=f32
                )
        r.cott[...] = r.cots[...].T
        gain, shift = gain2[...], shift2[...]

        def second_norm(at, i, _):
            for b in range(2):
                rows = rows_of(b, i)
                hat, rstd = standardized(r.xs[b, at, :].astype(f32) + r.hat2[rows, :])
                r.hat2[rows, :] = hat
                r.rstd2[rows, :] = jnp.broadcast_to(rstd, (16, 128))
                r.n2[rows, :] = jnp.where(real(i), hat * gain + shift, 0.0).astype(bf16)
            return 0

        blocks_of(13, 16, second_norm, group=3)
        r.n2t[...] = r.n2[...].T

    def forward(j):
        slot = remainder(j, 2)
        wait(weights(j))

        @pl.when(j + 1 < CHUNKS)
        def _():
            start(weights(j + 1))

        columns = pl.ds(pl.multiple_of(j * WIDTH, WIDTH), WIDTH)
        for b in range(WIDTH // 256):
            part = slice(256 * b, 256 * (b + 1))
            hid[:ROWS, part] = jnp.dot(r.n2[:ROWS, :], r.w_in[slot, :, part], preferred_element_type=f32)
            dact[:ROWS, part] = jnp.dot(r.cots[:ROWS, :], r.w_out[slot, :, part], preferred_element_type=f32)
        shift = bias2[:, columns]

        def rows(at, i, total):
            value, slope = gelu_parts(hid[at, :] + shift)
            act[at, :] = value.astype(bf16)
            d = (dact[at, :] * slope).astype(bf16)
            dhid[at, :] = d
            return total + jnp.sum(d.astype(f32).reshape(4, 8, WIDTH), axis=0)

        total = blocks_of(ROWS // 32, 32, rows, jnp.zeros((8, WIDTH), f32))
        early[pl.ds(j, 1), :WIDTH] = jnp.sum(total, axis=0, keepdims=True)

    def gradients(j):
        slot = remainder(j, 2)

        def rows(at, i, _):
            out = jnp.dot(r.cott[at, :], act[...], preferred_element_type=f32).reshape(2, 4, 2, 2, 8, WIDTH)
            r.own[0][i] = out[..., :384]
            r.own[1][i, :, :, :, :, :, :128] = out[..., 384:]
            inn = jnp.dot(r.n2t[at, :], dhid[...], preferred_element_type=f32).reshape(2, 4, 2, 2, 8, WIDTH)
            r.own[1][i, :, :, :, :, :, 128:] = inn[..., :256]
            r.own[2][i] = inn[..., 256:]
            return 0

        blocks_of(4, 256, rows)
        start(pair_copies(j))
        for b in range(4):
            part = slice(256 * b, 256 * (b + 1))
            dn2[:, part] += lax.dot_general(
                dhid[:ROWS, :],
                r.w_in[slot, part, :],
                (((1,), (1,)), ((), ())),
                preferred_element_type=f32,
            )

    def across(a, b):
        return lax.dot_general(a, b, (((1,), (1,)), ((), ())), preferred_element_type=f32)

    def fold_into(ref, row, lane, total):
        summed = jnp.sum(total, axis=0, keepdims=True)
        for k in range(4):
            ref[row + k : row + k + 1, lane : lane + 256] += summed[:, 256 * k : 256 * (k + 1)]

    def token_backward(b):
        gain = gain2[...]
        for half in range(2):
            dmr(b, half)[IMAGE:, :] = jnp.zeros((256 - IMAGE, 512), bf16)

        def second_norm(at, i, sums):
            rows = rows_of(b, i)
            hat, incoming = r.hat2[rows, :], dn2[rows, :]
            g = r.cots[rows, :].astype(f32)
            dmixed = g + norm_backward(incoming, hat, r.rstd2[rows, :1], gain)
            dn2[rows, :] = dmixed
            rounded = dmixed.astype(bf16)
            for half in range(2):
                dmr(b, half)[at, :] = rounded[:, columns_of(half)]
            r.columns[at, :] += jnp.broadcast_to(jnp.sum(dmixed, axis=1, keepdims=True), (16, 128))
            return (sums[0] + folded(incoming * hat), sums[1] + folded(incoming), sums[2] + folded(g))

        zero = jnp.zeros((8, 1024), f32)
        sums = blocks_of(13, 16, second_norm, (zero, zero, zero), group=2)
        fold_into(early, 0, 512, sums[0])
        fold_into(early, 4, 512, sums[1])
        fold_into(early, 0, 768, sums[2])
        for half in range(2):
            token_hidden(b, columns_of(half))
            dact[...] = jnp.dot(r.tout[...], dmr(b, half)[...], preferred_element_type=f32)

            def back(at, i, _):
                slope = gelu_parts(hid[at, :] + r.bias1[at, :1])[1]
                dh1(b, half)[at, :] = (dact[at, :] * slope).astype(bf16)
                return 0

            blocks_of(16, 32, back)

    def token_gradients(b):
        ones = jnp.ones((8, 512), bf16)
        for half in range(2):
            columns = columns_of(half)
            r.grad_tin[...] += across(dh1(b, half)[...], r.n1[b, :, columns])
            r.grad_tout[...] += across(r.act1[b, :, columns], dmr(b, half)[...])
            total = across(ones, dh1(b, half)[...])[:1]
            for k in range(4):
                late[k : k + 1, 256:] += total[:, 128 * k : 128 * (k + 1)]

    def send_token_gradients():
        for h, grad in enumerate((r.grad_tin, r.grad_tout)):
            r.own[2][:, :, :, :, h] = grad[...].reshape(4, 2, 4, 2, 8, 256)
        start(pair_copies(CHUNKS))

    def input_gradients(b):
        gain = gain1[...]
        for half in range(2):
            r.hat2[:IMAGE, columns_of(half)] = jnp.dot(
                r.tint[:IMAGE, :], dh1(b, half)[...], preferred_element_type=f32
            )

        def first_norm(at, i, sums):
            hat, rstd = standardized(r.xs[b, at, :].astype(f32))
            incoming = r.hat2[at, :]
            rows = rows_of(b, i)
            dn2[rows, :] += norm_backward(incoming, hat, rstd, gain)
            return (sums[0] + folded(incoming * hat), sums[1] + folded(incoming))

        zero = jnp.zeros((8, 1024), f32)
        sums = blocks_of(13, 16, first_norm, (zero, zero), group=2)
        fold_into(late, 0, 0, sums[0])
        fold_into(late, 4, 0, sums[1])

    def interleave():
        def rows(at, i, _):
            both = [dn2[pl.ds(pl.multiple_of(IMAGE * b + 8 * i, 8), 8), :] for b in range(2)]
            grad_inputs[pl.ds(pl.multiple_of(8 * i, 8), 8)] = jnp.stack(both, axis=1).astype(bf16)
            return 0

        blocks_of(24, 8, rows)
        both = [dn2[IMAGE * b + 192 : IMAGE * b + 200, :][: PATCHES - 192] for b in range(2)]
        grad_inputs[192:PATCHES] = jnp.stack(both, axis=1).astype(bf16)

    def sums_copies(which, step):
        at = (r.early, r.late)[which]
        send, recv = r.sums_send.at[which, step], r.sums_recv.at[which, step]
        if step == 0:
            return [remote(at[0], at[1], send.at[0], recv.at[0], device(core=1 - core))]
        axis, ring = AXES[step - 1], at[step + 1]
        return [
            remote(ring.at[0], ring.at[by], send.at[by - 1], recv.at[by - 1], device(**{axis: along(axis, by)}))
            for by in (1, 2, 3)
        ]

    def sums_stage(which, step):
        at = (r.early, r.late)[which]
        if step == 0:
            start(sums_copies(which, 0))
            return None
        wait(sums_copies(which, step - 1))
        if step == 1:
            total = at[0][...] + at[1][...]
        else:
            ring, mine = at[step], me[AXES[step - 2]]
            terms = [ring[remainder(mine + 4 - k, 4)] for k in range(4)]
            total = (terms[0] + terms[1]) + (terms[2] + terms[3])
        if step < 4:
            at[step + 1][0] = total
            start(sums_copies(which, step))
        return total

    def unfold(total, row, lane):
        return [total[row + k : row + k + 1, lane : lane + 256] for k in range(4)]

    def finish_early(total):
        for j in range(CHUNKS):
            grad_b2[:, WIDTH * j : WIDTH * (j + 1)] = total[j : j + 1, :WIDTH]
        for n, (row, lane) in ((2, (0, 512)), (3, (4, 512)), (4, (0, 768))):
            for k, part in enumerate(unfold(total, row, lane)):
                grad_norms[n : n + 1, 256 * k : 256 * (k + 1)] = part
        grad_bo[...] = total[4:5, 768 : 768 + PATCHES]

    def finish_late(total):
        for n, row in ((0, 0), (1, 4)):
            for k, part in enumerate(unfold(total, row, 0)):
                grad_norms[n : n + 1, 256 * k : 256 * (k + 1)] = part
        for k in range(4):
            grad_b1[:, 128 * k : 128 * (k + 1)] = total[k : k + 1, 256:]

    start(weights(jnp.int32(0)))
    for ref in (act, dhid):
        ref[ROWS:, :] = jnp.zeros((512 - ROWS, WIDTH), bf16)
    for ref in (dn2, early, late, r.columns, r.grad_tin, r.grad_tout):
        ref[...] = jnp.zeros(ref.shape, f32)
    prologue()
    pl.semaphore_wait(barrier, len(partners))

    def slot_of(t, _):
        chunk = lax.div(t, jnp.int32(2))

        @pl.when((t < AFTER) & (remainder(t, 2) == 0))
        def _():
            forward(chunk)

        @pl.when((t < AFTER) & (remainder(t, 2) == 1))
        def _():
            gradients(chunk)

        @pl.when((t >= AFTER) & (t < AFTER + 2))
        def _():
            token_backward(t - AFTER)

        @pl.when((t >= AFTER + 2) & (t < AFTER + 4))
        def _():
            token_gradients(t - AFTER - 2)

        @pl.when(t == AFTER + 3)
        def _():
            send_token_gradients()

        @pl.when((t >= AFTER + 4) & (t < AFTER + 6))
        def _():
            input_gradients(t - AFTER - 4)

        @pl.when(t == EARLY_SUMS)
        def _():
            early[4:5, 768:] = r.columns[...].T[:1, :]

        for step in range(4):
            for which, first in enumerate((EARLY_SUMS, LATE_SUMS)):

                @pl.when(t == first + step)
                def _():
                    sums_stage(which, step)

        serve(t)

        @pl.when(t == LATE_SUMS + 1)
        def _():
            interleave()

        return 0

    lax.fori_loop(0, SLOTS, slot_of, 0)
    finish_early(sums_stage(0, 4))
    finish_late(sums_stage(1, 4))
    for h in range(2):
        for j in range(CHUNKS):
            for g, out in enumerate((grad_out, grad_in)):
                out[8 * h : 8 * (h + 1), WIDTH * j : WIDTH * (j + 1)] = r.done[
                    h, j, :, WIDTH * g : WIDTH * (g + 1)
                ]
    grad_tin[...] = r.done_token[0, :, :PATCHES]
    grad_tout[...] = r.done_token[1, :, :PATCHES]


def hand_over(*refs):
    count = len(refs) // 2
    for source, target in zip(refs[:count], refs[count:]):
        target[...] = source[...]


def per_device(
    inputs,
    cotangent,
    first_gain,
    first_shift,
    token_in,
    token_in_bias,
    token_out,
    second_gain,
    second_shift,
    channel_in,
    channel_in_bias,
    channel_out,
):
    f32 = jnp.float32
    hidden = channel_in.shape[1]
    vmem, anywhere = pl.BlockSpec(memory_space=pltpu.VMEM), pl.BlockSpec(memory_space=pl.ANY)

    results = pl.pallas_call(
        block_kernel,
        out_shape=(
            jax.ShapeDtypeStruct((PATCHES, 2, 1024), jnp.bfloat16),
            jax.ShapeDtypeStruct((8, PATCHES), f32),
            jax.ShapeDtypeStruct((8, PATCHES), f32),
            jax.ShapeDtypeStruct((16, hidden), f32),
            jax.ShapeDtypeStruct((16, hidden), f32),
            jax.ShapeDtypeStruct((5, 1024), f32),
            jax.ShapeDtypeStruct((1, 512), f32),
            jax.ShapeDtypeStruct((1, PATCHES), f32),
            jax.ShapeDtypeStruct((1, hidden), f32),
        ),
        in_specs=[vmem] * 9 + [anywhere, vmem, anywhere],
        out_specs=(vmem,) * 9,
        scratch_shapes=(scratch_of(),),
        compiler_params=pltpu.CompilerParams(collective_id=0, has_side_effects=True, vmem_limit_bytes=67_000_000),
        name="block_backward",
    )(
        inputs.swapaxes(0, 1),
        cotangent.swapaxes(0, 1),
        first_gain.reshape(1, -1),
        first_shift.reshape(1, -1),
        token_in.T,
        token_in_bias.reshape(1, -1),
        token_out.T,
        second_gain.reshape(1, -1),
        second_shift.reshape(1, -1),
        channel_in,
        channel_in_bias.reshape(1, -1),
        channel_out,
    )
    results = pl.pallas_call(
        hand_over,
        out_shape=tuple(jax.ShapeDtypeStruct(a.shape, a.dtype) for a in results),
        in_specs=[vmem] * 9,
        out_specs=(vmem,) * 9,
        name="hand_over",
    )(*results)
    return (results[0].swapaxes(0, 1), *results[1:6], *(a[0] for a in results[6:]))


def solution(mesh):
    split = Mesh(
        mesh.devices.reshape(mesh.shape["grp"], 4, 2, 4, 2),
        ("grp", "dev_0", "dev_1", "dev_2", "dev_3"),
    )
    in_specs = (
        P(GRP_DEV, None, None),
        P(GRP_DEV, None, None),
        P(),
        P(),
        P(),
        P(),
        P(),
        P(),
        P(),
        P(),
        P(),
        P(),
    )
    out_specs = (
        P(GRP_DEV, None, None),
        P(DEV, None),
        P(DEV, None),
        P(DEV, None),
        P(DEV, None),
        P(),
        P(),
        P(),
        P(),
    )
    return jax.shard_map(
        per_device, mesh=split, in_specs=in_specs, out_specs=out_specs, check_vma=False
    )
```

```python
import math
from typing import Any, NamedTuple

import jax
import jax.numpy as jnp
from jax import lax
from jax.experimental import pallas as pl
from jax.experimental.pallas import tpu as pltpu
from jax.sharding import Mesh
from jax.sharding import PartitionSpec as P

DEV = ("dev_0", "dev_1", "dev_2", "dev_3")
GRP_DEV = ("grp", "dev_0", "dev_1", "dev_2", "dev_3")
MESH = pl.DeviceIdType.MESH

epsilon = 1e-06

AXES = ("x", "y", "z")
CHUNKS = 8
WIDTH = 512
IMAGE = 208
ROWS = 416
PATCHES = 196
COLOURS = (("x", "z", "y", 384), ("y", "z", "x", 384), ("z", "x", "y", 256))
FIRST = (0, 384, 768)
LAG = (0, 2, 5, 8, 11, 14, 17, 20)
AFTER = 2 * CHUNKS
LATE_SLOT = (0, 20, 22, 25, 27, 29, 32, 34)
SLOTS = 2 * (CHUNKS - 1) + LAG[-1] + 1
EARLY_SUMS = AFTER + 2
LATE_SUMS = AFTER + 6


def remainder(a, b):
    return lax.rem(a, jnp.int32(b))


def where_on(fixed, half=None):
    index = [slice(None)] * 4
    for axis, at in fixed.items():
        if axis == "x":
            index[0] = at
        elif axis == "y":
            index[2] = at
        else:
            index[1] = remainder(at, 2)
            index[3] = lax.div(at, jnp.int32(2))
    if half is not None:
        axis, part = half
        if axis == "z_lo":
            index[1] = part
        else:
            index[0 if axis == "x" else 2] = pl.ds(2 * part, 2)
    return tuple(index)


HALVES = (("z_lo", "y"), ("z_lo", "x"), ("x", "y"))
HALF_SHAPES = (((4, 2), (2,)), ((4, 2), (2,)), ((2, 4), (2,)))
BLOCK_SHAPES = (((2, 4, 2), (4,)), ((4, 2, 2), (4,)), ((4, 4), (4,)))


def gelu_parts(v):
    twice = 1.0 + lax.erf(v * (1.0 / math.sqrt(2.0)))
    value = 0.5 * v * twice
    slope = 0.5 * twice + v * jnp.exp(-0.5 * v * v) * (1.0 / math.sqrt(2.0 * math.pi))
    return value, slope


def standardized(values):
    centred = values - jnp.mean(values, axis=-1, keepdims=True)
    rstd = lax.rsqrt(jnp.mean(centred * centred, axis=-1, keepdims=True) + epsilon)
    return centred * rstd, rstd


def norm_backward(incoming, scaled, inv_std, gain):
    weighted = incoming * gain
    first_mean = jnp.mean(weighted, axis=-1, keepdims=True)
    second_mean = jnp.mean(weighted * scaled, axis=-1, keepdims=True)
    return inv_std * (weighted - first_mean - scaled * second_mean)


class Scratch(NamedTuple):
    own: Any
    sums: Any
    half: Any
    block: Any
    last: Any
    done: Any
    done_token: Any
    w_in: Any
    w_out: Any
    act: Any
    dhid: Any
    hid: Any
    dact: Any
    xs: Any
    n1: Any
    act1: Any
    hat2: Any
    rstd2: Any
    n2: Any
    n2t: Any
    cots: Any
    cott: Any
    tin: Any
    tint: Any
    tout: Any
    toutt: Any
    grad_tin: Any
    grad_tout: Any
    dn2: Any
    columns: Any
    bias1: Any
    early: Any
    late: Any
    w_sem: Any
    pair_send: Any
    pair_recv: Any
    half_send: Any
    half_recv: Any
    block_send: Any
    block_recv: Any
    last_send: Any
    last_recv: Any
    both_send: Any
    both_recv: Any
    sums_send: Any
    sums_recv: Any


def scratch_of():
    f32 = lambda *shape: pltpu.VMEM(shape, jnp.float32)
    bf16 = lambda *shape: pltpu.VMEM(shape, jnp.bfloat16)
    dma = lambda *shape: pltpu.SemaphoreType.DMA(shape)
    widths = [colour[3] for colour in COLOURS]
    chunks = [CHUNKS, CHUNKS, CHUNKS + 1]

    def received(shapes):
        return [
            [f32(chunks[c], 2, *shapes[c][p], 8, widths[c]) for p in range(2)] for c in range(3)
        ]

    return Scratch(
        own=[f32(4, 2, 4, 2, 2, 8, w) for w in widths],
        sums=[f32(chunks[c], 4, 2, 4, 2, 8, widths[c]) for c in range(3)],
        half=received(HALF_SHAPES),
        block=received(BLOCK_SHAPES),
        last=[f32(chunks[c], 3, 8, widths[c]) for c in range(3)],
        done=f32(2, CHUNKS, 8, 2 * WIDTH),
        done_token=f32(2, 8, 256),
        w_in=bf16(2, 1024, WIDTH),
        w_out=bf16(2, 1024, WIDTH),
        act=bf16(512, WIDTH),
        dhid=bf16(512, WIDTH),
        hid=f32(512, WIDTH),
        dact=f32(512, WIDTH),
        xs=bf16(2, IMAGE, 1024),
        n1=bf16(2, 256, 1024),
        act1=bf16(2, 512, 1024),
        hat2=f32(ROWS, 1024),
        rstd2=f32(ROWS, 128),
        n2=bf16(512, 1024),
        n2t=bf16(1024, 512),
        cots=bf16(512, 1024),
        cott=bf16(1024, 512),
        tin=bf16(512, 256),
        tint=bf16(256, 512),
        tout=bf16(512, 256),
        toutt=bf16(256, 512),
        grad_tin=f32(512, 256),
        grad_tout=f32(512, 256),
        dn2=f32(ROWS, 1024),
        columns=f32(256, 128),
        bias1=f32(512, 128),
        early=[f32(8, 1024), f32(8, 1024), *(f32(4, 8, 1024) for _ in AXES)],
        late=[f32(8, 384), f32(8, 384), *(f32(4, 8, 384) for _ in AXES)],
        w_sem=dma(2, 2),
        pair_send=dma(CHUNKS + 1, 3),
        pair_recv=dma(CHUNKS + 1, 3),
        half_send=[dma(CHUNKS + 1, 3, 2) for _ in range(2)],
        half_recv=[dma(CHUNKS + 1, 3, 2) for _ in range(2)],
        block_send=[dma(CHUNKS + 1, 3, 2) for _ in range(2)],
        block_recv=[dma(CHUNKS + 1, 3, 2) for _ in range(2)],
        last_send=dma(CHUNKS + 1, 3, 3),
        last_recv=dma(CHUNKS + 1, 3, 3),
        both_send=dma(CHUNKS + 1),
        both_recv=dma(CHUNKS + 1),
        sums_send=dma(2, 4, 3),
        sums_recv=dma(2, 4, 3),
    )


def block_kernel(*refs):
    inputs, cotangent, gain1, shift1, token_in, bias1, token_out, gain2, shift2, win, bias2, wout = refs[:12]
    grad_inputs, grad_tin, grad_tout, grad_in, grad_out, grad_norms, grad_b1, grad_bo, grad_b2 = refs[12:21]
    r = refs[21]
    f32, bf16 = jnp.float32, jnp.bfloat16
    x, y, core = lax.axis_index("dev_0"), lax.axis_index("dev_2"), lax.axis_index("dev_3")
    high = lax.axis_index("grp")
    me = {"x": x, "y": y, "z": 2 * high + lax.axis_index("dev_1")}

    def device(core=core, **moved):
        at = {**me, **moved}
        return (lax.div(at["z"], jnp.int32(2)), at["x"], remainder(at["z"], 2), at["y"], core)

    def along(axis, by):
        return remainder(me[axis] + by, 4)

    partners = [device(core=1 - core)]
    for axis in AXES:
        partners += [device(**{axis: along(axis, by)}) for by in (1, 2, 3)]
    barrier = pltpu.get_barrier_semaphore()
    for partner in partners:
        pl.semaphore_signal(barrier, inc=1, device_id=partner, device_id_type=MESH)

    def remote(source, target, send, recv, to):
        return pltpu.make_async_remote_copy(
            src_ref=source, dst_ref=target, send_sem=send, recv_sem=recv, device_id=to, device_id_type=MESH
        )

    def fixed_before(c, p):
        return {axis: me[axis] for axis in COLOURS[c][:p]}

    def colours(j):
        return (2,) if isinstance(j, int) else (0, 1, 2)

    def pair_copies(j):
        every = slice(None)
        return [
            remote(
                r.own[c].at[every, every, every, 1 - core],
                r.sums[c].at[j],
                r.pair_send.at[j, c],
                r.pair_recv.at[j, c],
                device(core=1 - core),
            )
            for c in colours(j)
        ]

    def half_copies(j, p):
        copies = []
        for c in colours(j):
            axis = COLOURS[c][p]
            for d, by in enumerate((1, 3)):
                spot = where_on({**fixed_before(c, p), axis: along(axis, 2)}, (HALVES[c][p], d))
                copies.append(
                    remote(
                        r.sums[c].at[(j, *spot)],
                        r.half[c][p].at[j, d],
                        r.half_send[p].at[j, c, d],
                        r.half_recv[p].at[j, c, d],
                        device(**{axis: along(axis, by)}),
                    )
                )
        return copies

    def block_copies(j, p):
        copies = []
        for c in colours(j):
            axis = COLOURS[c][p]
            for d, by in enumerate((1, 3)):
                spot = where_on({**fixed_before(c, p), axis: along(axis, by)})
                copies.append(
                    remote(
                        r.sums[c].at[(j, *spot)],
                        r.block[c][p].at[j, d],
                        r.block_send[p].at[j, c, d],
                        r.block_recv[p].at[j, c, d],
                        device(**{axis: along(axis, by)}),
                    )
                )
        return copies

    def last_copies(j):
        copies = []
        for c in colours(j):
            axis = COLOURS[c][2]
            for d, by in enumerate((1, 2, 3)):
                spot = where_on({**fixed_before(c, 2), axis: along(axis, by)})
                copies.append(
                    remote(
                        r.sums[c].at[(j, *spot)],
                        r.last[c].at[j, d],
                        r.last_send.at[j, c, d],
                        r.last_recv.at[j, c, d],
                        device(**{axis: along(axis, by)}),
                    )
                )
        return copies

    def both_copy(j):
        mine = r.done_token.at[high] if isinstance(j, int) else r.done.at[high, j]
        return remote(
            mine,
            mine,
            r.both_send.at[j],
            r.both_recv.at[j],
            device(z=along("z", 2)),
        )

    def start(copies):
        for copy in copies:
            copy.start()

    def wait(copies):
        for copy in copies:
            copy.wait()

    def stage(s, j):
        if s == 1:
            wait(pair_copies(j))
            for c in colours(j):
                for b in range(4):
                    r.sums[c][j, b] += r.own[c][b, :, :, core]
            start(half_copies(j, 0))
        elif s in (2, 4):
            p = s // 2 - 1
            wait(half_copies(j, p))
            for c in colours(j):
                axis = COLOURS[c][p]
                for d, by in enumerate((1, 3)):
                    spot = where_on({**fixed_before(c, p), axis: along(axis, by)}, (HALVES[c][p], d))
                    r.sums[c][(j, *spot)] += r.half[c][p][j, d]
            start(block_copies(j, p))
        elif s in (3, 5):
            p = s // 2 - 1
            wait(block_copies(j, p))
            for c in colours(j):
                spot = where_on(fixed_before(c, p + 1))
                r.sums[c][(j, *spot)] += r.block[c][p][j, 0] + r.block[c][p][j, 1]
            start(half_copies(j, 1) if p == 0 else last_copies(j))
        elif s == 6:
            wait(last_copies(j))
            for c in colours(j):
                width = COLOURS[c][3]
                spot = where_on(me)
                got = r.last[c]
                total = r.sums[c][(j, *spot)] + got[j, 0] + (got[j, 1] + got[j, 2])
                if isinstance(j, int):
                    r.done_token[high] = total
                else:
                    r.done[high, j, :, FIRST[c] : FIRST[c] + width] = total
            start([both_copy(j)])
        else:
            wait([both_copy(j)])

    def serve(t):
        for s in range(7, 0, -1):
            from_start = t - LAG[s]
            j = lax.div(from_start, jnp.int32(2))

            @pl.when((from_start >= 0) & (from_start < 2 * CHUNKS) & (remainder(from_start + 4 * CHUNKS, 2) == 0))
            def _():
                stage(s, j)

            @pl.when(t == LATE_SLOT[s])
            def _():
                stage(s, CHUNKS)

    def weights(j):
        slot = remainder(j, 2)
        columns = pl.ds(pl.multiple_of(j * WIDTH, WIDTH), WIDTH)
        return [
            pltpu.make_async_copy(win.at[:, columns], r.w_in.at[slot], r.w_sem.at[slot, 0]),
            pltpu.make_async_copy(wout.at[:, columns], r.w_out.at[slot], r.w_sem.at[slot, 1]),
        ]

    act, dhid, hid, dact, dn2 = r.act, r.dhid, r.hid, r.dact, r.dn2
    early, late = r.early[0], r.late[0]

    def blocks_of(count, size, step, carry=0, group=1):
        def at_block(i, carry):
            for u in range(group):
                n = i * group + u
                carry = step(pl.ds(pl.multiple_of(n * size, size), size), n, carry)
            return carry

        carry = lax.fori_loop(0, count // group, at_block, carry)
        for n in range(count // group * group, count):
            carry = step(pl.ds(n * size, size), n, carry)
        return carry

    def real(i):
        return lax.broadcasted_iota(jnp.int32, (16, 1), 0) + 16 * i < PATCHES

    def folded(values):
        return jnp.sum(values.reshape(2, 8, 1024), axis=0)

    def rows_of(b, i):
        return pl.ds(pl.multiple_of(IMAGE * b + 16 * i, 16), 16)

    def columns_of(half):
        return slice(512 * half, 512 * (half + 1))

    def dh1(b, half):
        return r.w_in.at[b, columns_of(half), :]

    def dmr(b, half):
        return r.w_out.at[b, 256 * half : 256 * (half + 1), :]

    def token_hidden(b, columns):
        hid[...] = jnp.dot(r.tin[...], r.n1[b, :, columns], preferred_element_type=f32)

    def both_images(ref, i, whole=True):
        if whole:
            values = ref[pl.ds(pl.multiple_of(16 * i, 16), 16)].astype(f32)
            return [values[:, b, :] for b in range(2)]
        values = ref[192:PATCHES].astype(f32)
        blocks = []
        for b in range(2):
            spot = r.hat2.at[16 * b : 16 * (b + 1), :]
            spot[...] = jnp.zeros((16, 1024), f32)
            spot[: PATCHES - 192, :] = values[:, b, :]
            blocks.append(spot[...])
        return blocks

    def prologue():
        for direct, turned, ref in ((r.tin, r.tint, token_in), (r.tout, r.toutt, token_out)):
            turned[192:, :] = jnp.zeros((64, 512), bf16)
            turned[:PATCHES, :] = ref[...]
            direct[...] = turned[...].T
        r.bias1[...] = jnp.broadcast_to(bias1[...], (128, 512)).T
        for b in range(2):
            r.n1[b, IMAGE:, :] = jnp.zeros((256 - IMAGE, 1024), bf16)
        gain, shift = gain1[...], shift1[...]

        def first_norm(at, i, _, whole=True):
            for b, values in enumerate(both_images(inputs, i, whole)):
                r.xs[b, at, :] = values.astype(bf16)
                value = standardized(values)[0] * gain + shift
                r.n1[b, at, :] = (value if whole else jnp.where(real(i), value, 0.0)).astype(bf16)
            return 0

        blocks_of(12, 16, first_norm, group=3)
        first_norm(pl.ds(192, 16), 12, 0, False)

        def split(at, i, _, whole=True):
            for b, values in enumerate(both_images(cotangent, i, whole)):
                r.cots[rows_of(b, i), :] = values.astype(bf16)
            return 0

        blocks_of(12, 16, split, group=3)
        split(None, 12, 0, False)
        r.cots[ROWS:, :] = jnp.zeros((512 - ROWS, 1024), bf16)
        r.n2[ROWS:, :] = jnp.zeros((512 - ROWS, 1024), bf16)
        for b in range(2):
            for half in range(2):
                columns = columns_of(half)
                token_hidden(b, columns)

                def activate(at, i, _):
                    value = gelu_parts(hid[at, :] + r.bias1[at, :1])[0]
                    r.act1[b, at, columns] = value.astype(bf16)
                    return 0

                blocks_of(16, 32, activate, group=4)
            for half in range(2):
                columns = columns_of(half)
                r.hat2[IMAGE * b : IMAGE * (b + 1), columns] = jnp.dot(
                    r.toutt[:IMAGE, :], r.act1[b, :, columns], preferred_element_type=f32
                )
        r.cott[...] = r.cots[...].T
        gain, shift = gain2[...], shift2[...]

        def second_norm(at, i, _):
            for b in range(2):
                rows = rows_of(b, i)
                hat, rstd = standardized(r.xs[b, at, :].astype(f32) + r.hat2[rows, :])
                r.hat2[rows, :] = hat
                r.rstd2[rows, :] = jnp.broadcast_to(rstd, (16, 128))
                r.n2[rows, :] = jnp.where(real(i), hat * gain + shift, 0.0).astype(bf16)
            return 0

        blocks_of(13, 16, second_norm, group=3)
        r.n2t[...] = r.n2[...].T

    def forward(j):
        slot = remainder(j, 2)
        wait(weights(j))

        @pl.when(j + 1 < CHUNKS)
        def _():
            start(weights(j + 1))

        columns = pl.ds(pl.multiple_of(j * WIDTH, WIDTH), WIDTH)
        for b in range(WIDTH // 256):
            part = slice(256 * b, 256 * (b + 1))
            hid[:ROWS, part] = jnp.dot(r.n2[:ROWS, :], r.w_in[slot, :, part], preferred_element_type=f32)
            dact[:ROWS, part] = jnp.dot(r.cots[:ROWS, :], r.w_out[slot, :, part], preferred_element_type=f32)
        shift = bias2[:, columns]

        def rows(at, i, total):
            value, slope = gelu_parts(hid[at, :] + shift)
            act[at, :] = value.astype(bf16)
            d = (dact[at, :] * slope).astype(bf16)
            dhid[at, :] = d
            return total + jnp.sum(d.astype(f32).reshape(4, 8, WIDTH), axis=0)

        total = blocks_of(ROWS // 32, 32, rows, jnp.zeros((8, WIDTH), f32), group=2)
        early[pl.ds(j, 1), :WIDTH] = jnp.sum(total, axis=0, keepdims=True)

    def gradients(j):
        slot = remainder(j, 2)

        def rows(at, i, _):
            out = jnp.dot(r.cott[at, :], act[...], preferred_element_type=f32).reshape(2, 4, 2, 2, 8, WIDTH)
            r.own[0][i] = out[..., :384]
            r.own[1][i, :, :, :, :, :, :128] = out[..., 384:]
            inn = jnp.dot(r.n2t[at, :], dhid[...], preferred_element_type=f32).reshape(2, 4, 2, 2, 8, WIDTH)
            r.own[1][i, :, :, :, :, :, 128:] = inn[..., :256]
            r.own[2][i] = inn[..., 256:]
            return 0

        blocks_of(4, 256, rows)
        start(pair_copies(j))
        for b in range(4):
            part = slice(256 * b, 256 * (b + 1))
            dn2[:, part] += lax.dot_general(
                dhid[:ROWS, :],
                r.w_in[slot, part, :],
                (((1,), (1,)), ((), ())),
                preferred_element_type=f32,
            )

    def across(a, b):
        return lax.dot_general(a, b, (((1,), (1,)), ((), ())), preferred_element_type=f32)

    def fold_into(ref, row, lane, total):
        summed = jnp.sum(total, axis=0, keepdims=True)
        for k in range(4):
            ref[row + k : row + k + 1, lane : lane + 256] += summed[:, 256 * k : 256 * (k + 1)]

    def token_backward(b):
        gain = gain2[...]
        for half in range(2):
            dmr(b, half)[IMAGE:, :] = jnp.zeros((256 - IMAGE, 512), bf16)

        def second_norm(at, i, sums):
            rows = rows_of(b, i)
            hat, incoming = r.hat2[rows, :], dn2[rows, :]
            g = r.cots[rows, :].astype(f32)
            dmixed = g + norm_backward(incoming, hat, r.rstd2[rows, :1], gain)
            dn2[rows, :] = dmixed
            rounded = dmixed.astype(bf16)
            for half in range(2):
                dmr(b, half)[at, :] = rounded[:, columns_of(half)]
            r.columns[at, :] += jnp.broadcast_to(jnp.sum(dmixed, axis=1, keepdims=True), (16, 128))
            return (sums[0] + folded(incoming * hat), sums[1] + folded(incoming), sums[2] + folded(g))

        zero = jnp.zeros((8, 1024), f32)
        sums = blocks_of(13, 16, second_norm, (zero, zero, zero), group=2)
        fold_into(early, 0, 512, sums[0])
        fold_into(early, 4, 512, sums[1])
        fold_into(early, 0, 768, sums[2])
        for half in range(2):
            token_hidden(b, columns_of(half))
            dact[...] = jnp.dot(r.tout[...], dmr(b, half)[...], preferred_element_type=f32)

            def back(at, i, _):
                slope = gelu_parts(hid[at, :] + r.bias1[at, :1])[1]
                dh1(b, half)[at, :] = (dact[at, :] * slope).astype(bf16)
                return 0

            blocks_of(16, 32, back, group=4)

    def token_gradients(b):
        ones = jnp.ones((8, 512), bf16)
        for half in range(2):
            columns = columns_of(half)
            r.grad_tin[...] += across(dh1(b, half)[...], r.n1[b, :, columns])
            r.grad_tout[...] += across(r.act1[b, :, columns], dmr(b, half)[...])
            total = across(ones, dh1(b, half)[...])[:1]
            for k in range(4):
                late[k : k + 1, 256:] += total[:, 128 * k : 128 * (k + 1)]

    def send_token_gradients():
        for h, grad in enumerate((r.grad_tin, r.grad_tout)):
            r.own[2][:, :, :, :, h] = grad[...].reshape(4, 2, 4, 2, 8, 256)
        start(pair_copies(CHUNKS))

    def input_gradients(b):
        gain = gain1[...]
        for half in range(2):
            r.hat2[:IMAGE, columns_of(half)] = jnp.dot(
                r.tint[:IMAGE, :], dh1(b, half)[...], preferred_element_type=f32
            )

        def first_norm(at, i, sums):
            hat, rstd = standardized(r.xs[b, at, :].astype(f32))
            incoming = r.hat2[at, :]
            rows = rows_of(b, i)
            dn2[rows, :] += norm_backward(incoming, hat, rstd, gain)
            return (sums[0] + folded(incoming * hat), sums[1] + folded(incoming))

        zero = jnp.zeros((8, 1024), f32)
        sums = blocks_of(13, 16, first_norm, (zero, zero), group=2)
        fold_into(late, 0, 0, sums[0])
        fold_into(late, 4, 0, sums[1])

    def interleave():
        def rows(at, i, _):
            both = [dn2[pl.ds(pl.multiple_of(IMAGE * b + 8 * i, 8), 8), :] for b in range(2)]
            grad_inputs[pl.ds(pl.multiple_of(8 * i, 8), 8)] = jnp.stack(both, axis=1).astype(bf16)
            return 0

        blocks_of(24, 8, rows)
        both = [dn2[IMAGE * b + 192 : IMAGE * b + 200, :][: PATCHES - 192] for b in range(2)]
        grad_inputs[192:PATCHES] = jnp.stack(both, axis=1).astype(bf16)

    def sums_copies(which, step):
        at = (r.early, r.late)[which]
        send, recv = r.sums_send.at[which, step], r.sums_recv.at[which, step]
        if step == 0:
            return [remote(at[0], at[1], send.at[0], recv.at[0], device(core=1 - core))]
        axis, ring = AXES[step - 1], at[step + 1]
        return [
            remote(ring.at[0], ring.at[by], send.at[by - 1], recv.at[by - 1], device(**{axis: along(axis, by)}))
            for by in (1, 2, 3)
        ]

    def sums_stage(which, step):
        at = (r.early, r.late)[which]
        if step == 0:
            start(sums_copies(which, 0))
            return None
        wait(sums_copies(which, step - 1))
        if step == 1:
            total = at[0][...] + at[1][...]
        else:
            ring, mine = at[step], me[AXES[step - 2]]
            terms = [ring[remainder(mine + 4 - k, 4)] for k in range(4)]
            total = (terms[0] + terms[1]) + (terms[2] + terms[3])
        if step < 4:
            at[step + 1][0] = total
            start(sums_copies(which, step))
        return total

    def unfold(total, row, lane):
        return [total[row + k : row + k + 1, lane : lane + 256] for k in range(4)]

    def finish_early(total):
        for j in range(CHUNKS):
            grad_b2[:, WIDTH * j : WIDTH * (j + 1)] = total[j : j + 1, :WIDTH]
        for n, (row, lane) in ((2, (0, 512)), (3, (4, 512)), (4, (0, 768))):
            for k, part in enumerate(unfold(total, row, lane)):
                grad_norms[n : n + 1, 256 * k : 256 * (k + 1)] = part
        grad_bo[...] = total[4:5, 768 : 768 + PATCHES]

    def finish_late(total):
        for n, row in ((0, 0), (1, 4)):
            for k, part in enumerate(unfold(total, row, 0)):
                grad_norms[n : n + 1, 256 * k : 256 * (k + 1)] = part
        for k in range(4):
            grad_b1[:, 128 * k : 128 * (k + 1)] = total[k : k + 1, 256:]

    start(weights(jnp.int32(0)))
    for ref in (act, dhid):
        ref[ROWS:, :] = jnp.zeros((512 - ROWS, WIDTH), bf16)
    for ref in (dn2, early, late, r.columns, r.grad_tin, r.grad_tout):
        ref[...] = jnp.zeros(ref.shape, f32)
    prologue()
    pl.semaphore_wait(barrier, len(partners))

    def slot_of(t, _):
        chunk = lax.div(t, jnp.int32(2))

        @pl.when((t < AFTER) & (remainder(t, 2) == 0))
        def _():
            forward(chunk)

        @pl.when((t < AFTER) & (remainder(t, 2) == 1))
        def _():
            gradients(chunk)

        @pl.when((t >= AFTER) & (t < AFTER + 2))
        def _():
            token_backward(t - AFTER)

        @pl.when((t >= AFTER + 2) & (t < AFTER + 4))
        def _():
            token_gradients(t - AFTER - 2)

        @pl.when(t == AFTER + 3)
        def _():
            send_token_gradients()

        @pl.when((t >= AFTER + 4) & (t < AFTER + 6))
        def _():
            input_gradients(t - AFTER - 4)

        @pl.when(t == EARLY_SUMS)
        def _():
            early[4:5, 768:] = r.columns[...].T[:1, :]

        for step in range(4):
            for which, first in enumerate((EARLY_SUMS, LATE_SUMS)):

                @pl.when(t == first + step)
                def _():
                    sums_stage(which, step)

        serve(t)

        @pl.when(t == LATE_SUMS + 1)
        def _():
            interleave()

        return 0

    lax.fori_loop(0, SLOTS, slot_of, 0)
    finish_early(sums_stage(0, 4))
    finish_late(sums_stage(1, 4))
    for h in range(2):
        for j in range(CHUNKS):
            for g, out in enumerate((grad_out, grad_in)):
                out[8 * h : 8 * (h + 1), WIDTH * j : WIDTH * (j + 1)] = r.done[
                    h, j, :, WIDTH * g : WIDTH * (g + 1)
                ]
    grad_tin[...] = r.done_token[0, :, :PATCHES]
    grad_tout[...] = r.done_token[1, :, :PATCHES]


def hand_over(*refs):
    count = len(refs) // 2
    for source, target in zip(refs[:count], refs[count:]):
        target[...] = source[...]


def per_device(
    inputs,
    cotangent,
    first_gain,
    first_shift,
    token_in,
    token_in_bias,
    token_out,
    second_gain,
    second_shift,
    channel_in,
    channel_in_bias,
    channel_out,
):
    f32 = jnp.float32
    hidden = channel_in.shape[1]
    vmem, anywhere = pl.BlockSpec(memory_space=pltpu.VMEM), pl.BlockSpec(memory_space=pl.ANY)

    results = pl.pallas_call(
        block_kernel,
        out_shape=(
            jax.ShapeDtypeStruct((PATCHES, 2, 1024), jnp.bfloat16),
            jax.ShapeDtypeStruct((8, PATCHES), f32),
            jax.ShapeDtypeStruct((8, PATCHES), f32),
            jax.ShapeDtypeStruct((16, hidden), f32),
            jax.ShapeDtypeStruct((16, hidden), f32),
            jax.ShapeDtypeStruct((5, 1024), f32),
            jax.ShapeDtypeStruct((1, 512), f32),
            jax.ShapeDtypeStruct((1, PATCHES), f32),
            jax.ShapeDtypeStruct((1, hidden), f32),
        ),
        in_specs=[vmem] * 9 + [anywhere, vmem, anywhere],
        out_specs=(vmem,) * 9,
        scratch_shapes=(scratch_of(),),
        compiler_params=pltpu.CompilerParams(collective_id=0, has_side_effects=True, vmem_limit_bytes=67_000_000),
        name="block_backward",
    )(
        inputs.swapaxes(0, 1),
        cotangent.swapaxes(0, 1),
        first_gain.reshape(1, -1),
        first_shift.reshape(1, -1),
        token_in.T,
        token_in_bias.reshape(1, -1),
        token_out.T,
        second_gain.reshape(1, -1),
        second_shift.reshape(1, -1),
        channel_in,
        channel_in_bias.reshape(1, -1),
        channel_out,
    )
    results = pl.pallas_call(
        hand_over,
        out_shape=tuple(jax.ShapeDtypeStruct(a.shape, a.dtype) for a in results),
        in_specs=[vmem] * 9,
        out_specs=(vmem,) * 9,
        name="hand_over",
    )(*results)
    return (results[0].swapaxes(0, 1), *results[1:6], *(a[0] for a in results[6:]))


def solution(mesh):
    split = Mesh(
        mesh.devices.reshape(mesh.shape["grp"], 4, 2, 4, 2),
        ("grp", "dev_0", "dev_1", "dev_2", "dev_3"),
    )
    in_specs = (
        P(GRP_DEV, None, None),
        P(GRP_DEV, None, None),
        P(),
        P(),
        P(),
        P(),
        P(),
        P(),
        P(),
        P(),
        P(),
        P(),
    )
    out_specs = (
        P(GRP_DEV, None, None),
        P(DEV, None),
        P(DEV, None),
        P(DEV, None),
        P(DEV, None),
        P(),
        P(),
        P(),
        P(),
    )
    return jax.shard_map(
        per_device, mesh=split, in_specs=in_specs, out_specs=out_specs, check_vma=False
    )
```
